128 devices in a mesh: grp: 4 (over z), seq: 32 (over x, y, core).
Axes of the slice: x: 4, y: 4, z: 4, core: 2. Of those that a mesh axis runs over, the one named last changes fastest.
Arguments:
- latent: bfloat16 [4, 4096, 32, 256], P('grp', 'seq'), may hold values from -6 to 6
- up_key: bfloat16 [4, 128, 256], replicated, may hold values from -0.5 to 0.5
- up_value: bfloat16 [4, 128, 256], replicated, may hold values from -0.5 to 0.5
- queries: bfloat16 [8, 64, 128], replicated, may hold values from -240 to 240, as said below
- lengths: int32 [8], replicated, may hold values from 1 to 16384
- block_dest: int32 [4096], replicated, may hold values from 0 to 127, as said below
Outputs:
- decode_latent: bfloat16 [128, 4, 32, 32, 256], P(('grp', 'seq'))
- attended: float32 [8, 8192], replicated
The draws below stay inside these ranges and needn't reach their ends.
Inputs may be any that keep to these rules, and one draw needn't show every extreme that they name: `block_dest`: each aligned run of 128 entries (the blocks of one seq index in the prefill layout) names every decode device exactly once. `queries`: the new token's query entries, real-valued.
All inputs are finite; a program needn't handle non-finite values.
Results may differ from the reference program's by a relative error of at most 0.001.
Values may be sent and summed in bfloat16 or wider, within the bound.
No kernel may reach another device: no remote copies, remote signals or barrier semaphores. Data moves between devices by JAX's collectives and lax.ppermute only.
A program may use at most 64 MiB of HBM per device.

```python
import jax
import jax.numpy as jnp
from jax import lax

Q_HEADS = 64
KV_HEADS = 8
HEAD_DIM = 128
RANK = 128
BATCH = 8
BT = 32
GROUPS = 4
DESTS = 128
BLOCKS = 4096
S_MAX = 16384


def draw_queries(key, part):
    drawn = jnp.clip(jax.random.normal(key, (BATCH, Q_HEADS, HEAD_DIM), jnp.float32), -4.0, 4.0)
    return drawn.astype(jnp.bfloat16)


def draw_block_dest(key, part):
    shards = BLOCKS // DESTS
    subkeys = jax.random.split(jax.random.fold_in(key, 11), shards)
    orders = jax.vmap(lambda subkey: jax.random.permutation(subkey, DESTS))(subkeys)
    return orders.reshape(BLOCKS).astype(jnp.int32)


def place_ends(values, key, least, largest):
    place = [jax.random.randint(jax.random.fold_in(key, axis), (), 0, length) for axis, length in enumerate(values.shape)]
    main_axis = values.shape.index(max(values.shape))
    next_to = place[:main_axis] + [(place[main_axis] + 1) % values.shape[main_axis]] + place[main_axis + 1:]
    return values.at[tuple(place)].set(least).at[tuple(next_to)].set(largest)


def steps_of(stream_key, shape, cuts, smallest, high):
    loudness = 1.0
    for position, blocks in cuts:
        steps = jax.random.uniform(jax.random.fold_in(jax.random.fold_in(stream_key, 6), position), (blocks,), jnp.float32, smallest / len(cuts), high / len(cuts))
        loudness = loudness * jnp.repeat(jnp.exp(steps), shape[position] // blocks).reshape((-1,) + (1,) * (len(shape) - 1 - position))
    return loudness


def noise(key, extent, spread, bound, pieces=(), kind=jnp.bfloat16):
    entries = spread * jax.random.normal(key, extent, jnp.float32)
    if pieces:
        entries = entries * steps_of(key, extent, pieces, -0.22, 0.18)
    return jnp.clip(entries, -bound, bound).astype(kind)


def setup_inputs(seed: int = 0) -> dict:
    streams_of = jax.random.split(jax.random.key(seed), 7)
    latent = noise(streams_of[0], (GROUPS, BLOCKS, BT, 2 * RANK), 1.0, 6.0, ((0, 4), (1, 32)))
    up_key = noise(streams_of[1], (GROUPS, RANK, KV_HEADS // GROUPS * HEAD_DIM), RANK ** -0.5, 0.5)
    up_value = noise(streams_of[2], (GROUPS, RANK, KV_HEADS // GROUPS * HEAD_DIM), RANK ** -0.5, 0.5)
    queries = draw_queries(jax.random.fold_in(streams_of[6], 71), 0)
    lengths = place_ends(jax.random.randint(streams_of[4], (BATCH,), 1, S_MAX + 1), jax.random.fold_in(streams_of[4], 1), 1, S_MAX).astype(jnp.int32)
    block_dest = draw_block_dest(jax.random.fold_in(streams_of[6], 71), 0)
    return dict(latent=latent, up_key=up_key, up_value=up_value, queries=queries, lengths=lengths, block_dest=block_dest)


def reference(latent, up_key, up_value, queries, lengths, block_dest):
    shards = BLOCKS // DESTS
    table = block_dest.reshape(shards, DESTS)
    row_ids = jnp.broadcast_to(jnp.arange(shards, dtype=jnp.int32)[:, None], (shards, DESTS))
    col_ids = jnp.broadcast_to(jnp.arange(DESTS, dtype=jnp.int32)[None, :], (shards, DESTS))
    source_order = jnp.zeros((shards, DESTS), jnp.int32).at[row_ids, table].set(col_ids)
    global_ids = row_ids * DESTS + source_order
    picked = latent[:, global_ids.T]
    decode_latent = jnp.transpose(picked, (1, 0, 2, 3, 4))
    per_group = KV_HEADS // GROUPS
    per_kv = Q_HEADS // KV_HEADS
    scale = 1.0 / math_sqrt(HEAD_DIM)
    query_f = queries.astype(jnp.float32).reshape(BATCH, GROUPS, per_group, per_kv, HEAD_DIM)
    positions = jnp.arange(S_MAX, dtype=jnp.int32)
    valid = positions[None, :] < lengths[:, None]

    def one_group(index):
        lat = lax.dynamic_index_in_dim(latent, index, 0, keepdims=False).astype(jnp.float32)
        lat = lat.reshape(BATCH, S_MAX, 2 * RANK)
        key_map = lax.dynamic_index_in_dim(up_key, index, 0, keepdims=False).astype(jnp.float32)
        value_map = lax.dynamic_index_in_dim(up_value, index, 0, keepdims=False).astype(jnp.float32)
        keys = jnp.einsum('bsr,rc->bsc', lat[..., :RANK], key_map, precision=lax.Precision.HIGHEST)
        values = jnp.einsum('bsr,rc->bsc', lat[..., RANK:], value_map, precision=lax.Precision.HIGHEST)
        keys = keys.reshape(BATCH, S_MAX, per_group, HEAD_DIM)
        values = values.reshape(BATCH, S_MAX, per_group, HEAD_DIM)
        query_g = lax.dynamic_index_in_dim(query_f, index, 1, keepdims=False)
        scores = jnp.einsum('bkjd,bskd->bkjs', query_g, keys, precision=lax.Precision.HIGHEST) * scale
        live = valid[:, None, None, :]
        scores = jnp.where(live, scores, -1e+30)
        row_max = lax.optimization_barrier(jnp.max(scores, axis=-1, keepdims=True))
        weights = jnp.where(live, jnp.exp(scores - row_max), 0.0)
        totals = lax.optimization_barrier(jnp.sum(weights, axis=-1))
        summed = jnp.einsum('bkjs,bskd->bkjd', weights, values, precision=lax.Precision.HIGHEST)
        return summed / totals[..., None]
    outputs = lax.map(one_group, jnp.arange(GROUPS, dtype=jnp.int32))
    attended = jnp.transpose(outputs, (1, 0, 2, 3, 4)).reshape(BATCH, Q_HEADS * HEAD_DIM)
    return (decode_latent, attended)

def math_sqrt(value):
    return float(value) ** 0.5
```

```python
import jax
import jax.numpy as jnp
from jax import lax
from jax.experimental import pallas as pl
from jax.experimental.pallas import tpu as pltpu
from jax.sharding import Mesh
from jax.sharding import PartitionSpec as P

SEQ = ("seq_0", "seq_1", "seq_2")
GRP_SEQ = ("grp", "seq_0", "seq_1", "seq_2")
NEG = -1e30


def slot_kernel(dests, latent, out, table, sem, sems):
    count = latent.shape[0]
    shard = lax.axis_index(SEQ)
    first = pltpu.make_async_copy(dests.at[pl.ds(shard * count, count)], table, sem)
    first.start()
    first.wait()

    def send(b, carry):
        pltpu.make_async_copy(latent.at[b], out.at[table[b]], sems).start()
        return carry

    lax.fori_loop(0, count, send, 0, unroll=8)
    pltpu.make_async_copy(latent, out, sems).wait()


def slotted(latent, dests):
    count = latent.shape[0]
    return pl.pallas_call(
        slot_kernel,
        out_shape=jax.ShapeDtypeStruct(latent.shape, latent.dtype),
        in_specs=[pl.BlockSpec(memory_space=pl.ANY), pl.BlockSpec(memory_space=pl.ANY)],
        out_specs=pl.BlockSpec(memory_space=pl.ANY),
        scratch_shapes=[
            pltpu.SMEM((count,), jnp.int32),
            pltpu.SemaphoreType.DMA,
            pltpu.SemaphoreType.DMA,
        ],
        name="slot",
    )(dests, latent)


def split(x, parts):
    pieces = []
    for _ in range(parts):
        piece = x.astype(jnp.bfloat16)
        pieces.append(piece)
        x = x - piece.astype(jnp.float32)
    return pieces


def attend_kernel(lengths, latent, up_key, queries, out):
    blocks, block_len, width = latent.shape
    rank = width // 2
    tokens = blocks * block_len
    heads = out.shape[1]
    head_dim = queries.shape[2]
    per_group = up_key.shape[2] // head_dim
    per_kv = heads // per_group
    shard = lax.axis_index(SEQ)
    group = lax.axis_index("grp")
    quarter = lax.axis_size(SEQ) // queries.shape[0]
    seq = shard // quarter
    live_count = lengths[seq] - (shard % quarter) * tokens
    query = queries[seq, pl.ds(pl.multiple_of(group * heads, heads), heads), :]
    query = query.astype(jnp.float32)
    key_map = up_key[group].astype(jnp.float32)
    rows = []
    for k in range(per_group):
        rows.append(
            lax.dot_general(
                query[k * per_kv : (k + 1) * per_kv].astype(jnp.bfloat16),
                key_map[:, k * head_dim : (k + 1) * head_dim].astype(jnp.bfloat16),
                (((1,), (1,)), ((), ())),
                preferred_element_type=jnp.float32,
            )
        )
    absorbed = jnp.concatenate(rows, axis=0) * (1.0 / float(head_dim) ** 0.5)
    lat = latent[...].reshape(tokens, width)
    parts = jnp.concatenate([p.astype(jnp.float32) for p in split(absorbed, 3)], axis=0)
    raw = lax.dot_general(
        parts.astype(jnp.bfloat16),
        lat[:, :rank],
        (((1,), (1,)), ((), ())),
        preferred_element_type=jnp.float32,
    )
    scores = raw[2 * heads :] + raw[heads : 2 * heads] + raw[:heads]
    live = lax.broadcasted_iota(jnp.int32, (heads, tokens), 1) < live_count
    scores = jnp.where(live, scores, NEG)
    largest = jnp.max(scores, axis=1, keepdims=True)
    weights = jnp.where(live, jnp.exp(scores - largest), 0.0)
    total = jnp.sum(weights, axis=1, keepdims=True)
    halves = jnp.concatenate([p.astype(jnp.float32) for p in split(weights, 2)], axis=0)
    summed = lax.dot_general(
        halves.astype(jnp.bfloat16),
        lat[:, rank:],
        (((1,), (0,)), ((), ())),
        preferred_element_type=jnp.float32,
    )
    out[0] = summed[:heads] + summed[heads:]
    out[1] = jnp.broadcast_to(largest, (heads, rank))
    out[2] = jnp.broadcast_to(total, (heads, rank))


def attend(latent, up_key, queries, lengths, heads):
    rank = latent.shape[2] // 2
    vmem = pl.BlockSpec(memory_space=pltpu.VMEM)
    return pl.pallas_call(
        attend_kernel,
        out_shape=jax.ShapeDtypeStruct((3, heads, rank), jnp.float32),
        in_specs=[pl.BlockSpec(memory_space=pltpu.SMEM), vmem, vmem, vmem],
        out_specs=vmem,
        name="attend",
    )(lengths, latent, up_key, queries)


def joined(first, second):
    largest = jnp.maximum(first[1], second[1])
    factor_a = jnp.exp(first[1] - largest)
    factor_b = jnp.exp(second[1] - largest)
    return jnp.stack(
        [
            first[0] * factor_a + second[0] * factor_b,
            largest,
            first[2] * factor_a + second[2] * factor_b,
        ]
    )


def finish_kernel(mine, theirs, up_value, out):
    heads = out.shape[0]
    head_dim = out.shape[1]
    per_group = up_value.shape[2] // head_dim
    per_kv = heads // per_group
    both = joined(mine, theirs)
    mean = both[0] / both[2]
    parts = jnp.concatenate([p.astype(jnp.float32) for p in split(mean, 3)], axis=0)
    wide = lax.dot_general(
        parts.astype(jnp.bfloat16),
        up_value[lax.axis_index("grp")],
        (((1,), (0,)), ((), ())),
        preferred_element_type=jnp.float32,
    )
    full = wide[2 * heads :] + wide[heads : 2 * heads] + wide[:heads]
    for k in range(per_group):
        rows = slice(k * per_kv, (k + 1) * per_kv)
        out[rows, :] = full[rows, k * head_dim : (k + 1) * head_dim]


def finish(mine, theirs, up_value, head_dim):
    vmem = pl.BlockSpec(memory_space=pltpu.VMEM)
    return pl.pallas_call(
        finish_kernel,
        out_shape=jax.ShapeDtypeStruct((mine.shape[1], head_dim), jnp.float32),
        in_specs=[vmem, vmem, vmem],
        out_specs=vmem,
        name="finish",
    )(mine, theirs, up_value)


def swap(x, axis, mask):
    return lax.ppermute(x, axis, [(i, i ^ mask) for i in range(lax.axis_size(axis))])


def body(latent, up_key, up_value, queries, lengths, block_dest):
    groups = up_key.shape[0]
    dests = latent.shape[1]
    batch, q_heads, head_dim = queries.shape
    heads = q_heads // groups
    outgoing = slotted(latent[0], block_dest)
    received = lax.all_to_all(outgoing, GRP_SEQ, split_axis=0, concat_axis=0, tiled=True)
    decode_latent = received.reshape(1, groups, dests // groups, *latent.shape[2:])

    partial = attend(latent[0], up_key, queries, lengths, heads)
    partial = joined(partial, swap(partial, "seq_2", 1))
    block = finish(partial, swap(partial, "seq_1", 1), up_value, head_dim)[None]
    own = {axis: lax.axis_index(axis) for axis in ("grp", "seq_0", "seq_1")}
    for axis, masks in (("seq_1", (3,)), ("seq_0", (1, 3)), ("grp", (1, 3))):
        for mask in masks:
            block = jnp.concatenate([block, swap(block, axis, mask)])
    g = jnp.arange(groups)[None, :]
    seq = jnp.arange(batch)[:, None]

    def place(wanted, here):
        high = (wanted >> 1) ^ (here >> 1)
        return 2 * high + ((wanted ^ here) & 1 ^ high)

    at = (
        place(g, own["grp"]) * 8
        + place(seq >> 1, own["seq_0"]) * 2
        + ((seq & 1) ^ (own["seq_1"] >> 1))
    )
    attended = block[at].reshape(batch, q_heads * head_dim)
    return (decode_latent, attended)


def solution(mesh):
    finer = Mesh(
        mesh.devices.reshape(mesh.shape["grp"], 4, 4, 2), ("grp", "seq_0", "seq_1", "seq_2")
    )
    in_specs = (P("grp", SEQ, None, None), P(), P(), P(), P(), P())
    out_specs = (P(GRP_SEQ, None, None, None, None), P())
    return jax.shard_map(body, mesh=finer, in_specs=in_specs, out_specs=out_specs, check_vma=False)
```

```python
import jax
import jax.numpy as jnp
from jax import lax
from jax.experimental import pallas as pl
from jax.experimental.pallas import tpu as pltpu
from jax.sharding import Mesh
from jax.sharding import PartitionSpec as P

SEQ = ("seq_0", "seq_1", "seq_2")
GRP_SEQ = ("grp", "seq_0", "seq_1", "seq_2")
NEG = -1e30
VMEM = pl.BlockSpec(memory_space=pltpu.VMEM)
SMEM = pl.BlockSpec(memory_space=pltpu.SMEM)
PARAMS = pltpu.CompilerParams(vmem_limit_bytes=16 << 20)


def split(x, parts):
    pieces = []
    for _ in range(parts):
        piece = x.astype(jnp.bfloat16).astype(jnp.float32)
        pieces.append(piece)
        x = x - piece
    return jnp.concatenate(pieces, axis=0).astype(jnp.bfloat16)


def attend_kernel(lengths, latent, up_key, queries, out):
    blocks, block_len, width = latent.shape
    rank = width // 2
    tokens = blocks * block_len
    heads = out.shape[1]
    head_dim = queries.shape[2]
    per_group = up_key.shape[2] // head_dim
    per_kv = heads // per_group
    shard = lax.axis_index(SEQ)
    group = lax.axis_index("grp")
    quarter = lax.axis_size(SEQ) // queries.shape[0]
    seq = shard // quarter
    live_count = lengths[seq] - (shard % quarter) * tokens
    query = queries[seq, pl.ds(pl.multiple_of(group * heads, heads), heads), :]
    query = query.astype(jnp.float32)
    key_map = up_key[group]
    rows = [
        lax.dot_general(
            query[k * per_kv : (k + 1) * per_kv].astype(jnp.bfloat16),
            key_map[:, k * head_dim : (k + 1) * head_dim],
            (((1,), (1,)), ((), ())),
            preferred_element_type=jnp.float32,
        )
        for k in range(per_group)
    ]
    absorbed = jnp.concatenate(rows, axis=0) * (1.0 / float(head_dim) ** 0.5)
    lat = latent[...].reshape(tokens, width)
    raw = lax.dot_general(
        split(absorbed, 3),
        lat[:, :rank],
        (((1,), (1,)), ((), ())),
        preferred_element_type=jnp.float32,
    )
    scores = raw[2 * heads :] + raw[heads : 2 * heads] + raw[:heads]
    live = lax.broadcasted_iota(jnp.int32, (heads, tokens), 1) < live_count
    scores = jnp.where(live, scores, NEG)
    largest = jnp.max(scores, axis=1, keepdims=True)
    weights = jnp.where(live, jnp.exp(scores - largest), 0.0)
    total = jnp.sum(weights, axis=1, keepdims=True)
    summed = lax.dot_general(
        split(weights, 2),
        lat[:, rank:],
        (((1,), (0,)), ((), ())),
        preferred_element_type=jnp.float32,
    )
    out[0] = summed[:heads] + summed[heads:]
    out[1] = jnp.broadcast_to(largest, (heads, rank))
    out[2] = jnp.broadcast_to(total, (heads, rank))


def attend(latent, up_key, queries, lengths, heads):
    rank = latent.shape[2] // 2
    return pl.pallas_call(
        attend_kernel,
        out_shape=jax.ShapeDtypeStruct((3, heads, rank), jnp.float32),
        in_specs=[SMEM, VMEM, VMEM, VMEM],
        out_specs=VMEM,
        compiler_params=PARAMS,
        name="attend",
    )(lengths, latent, up_key, queries)


def joined(first, second):
    largest = jnp.maximum(first[1], second[1])
    factor_a = jnp.exp(first[1] - largest)
    factor_b = jnp.exp(second[1] - largest)
    accum = first[0] * factor_a + second[0] * factor_b
    return (accum, largest, first[2] * factor_a + second[2] * factor_b)


def merge_kernel(mine, theirs, out):
    kept = out.shape[1]
    rows = pl.ds(pl.multiple_of(lax.axis_index("seq_2") * kept, kept), kept)
    both = joined(
        [mine[i, rows, :] for i in range(3)], [theirs[i, rows, :] for i in range(3)]
    )
    for i in range(3):
        out[i] = both[i]


def merge(mine, theirs):
    return pl.pallas_call(
        merge_kernel,
        out_shape=jax.ShapeDtypeStruct((3, mine.shape[1] // 2, mine.shape[2]), jnp.float32),
        in_specs=[VMEM, VMEM],
        out_specs=VMEM,
        compiler_params=PARAMS,
        name="merge",
    )(mine, theirs)


def pack_kernel(table, latent, mine, theirs, up_value, out):
    blocks, block_len, width = latent.shape
    rank = width // 2
    head_dim = mine.shape[2]
    accum, _, total = joined([mine[i] for i in range(3)], [theirs[i] for i in range(3)])
    mean = accum / total
    half = mean.shape[0] // 2
    mean = jnp.where(lax.axis_index("seq_1") % 2 == 1, mean[half:], mean[:half])
    value_map = up_value[lax.axis_index("grp")]
    value_map = jnp.where(
        lax.axis_index("seq_2") == 1, value_map[:, head_dim:], value_map[:, :head_dim]
    )
    wide = lax.dot_general(
        split(mean, 3), value_map, (((1,), (0,)), ((), ())), preferred_element_type=jnp.float32
    )
    extra = split(wide[2 * half :] + wide[half : 2 * half] + wide[:half], 2)

    def place(b, carry):
        to = table[b]
        out[to, :block_len, :] = latent[b, :, :rank]
        out[to, block_len : 2 * block_len, :] = latent[b, :, rank:]
        out[b, 2 * block_len :, :] = extra
        return carry

    lax.fori_loop(0, blocks, place, 0, unroll=4)


def pack(table, latent, mine, theirs, up_value):
    blocks, block_len, width = latent.shape
    rows = 2 * block_len + mine.shape[1]
    return pl.pallas_call(
        pack_kernel,
        out_shape=jax.ShapeDtypeStruct((blocks, rows, width // 2), latent.dtype),
        in_specs=[SMEM, VMEM, VMEM, VMEM, VMEM],
        out_specs=VMEM,
        compiler_params=PARAMS,
        name="pack",
    )(table, latent, mine, theirs, up_value)


def unpack_kernel(received, decode, attended, sems):
    sources, rows, rank = received.shape
    _, _, _, block_len, _ = decode.shape
    groups = lax.axis_size("grp")
    shards = sources // groups
    copies = []
    for g in range(groups):
        for k in range(2):
            copies.append(
                pltpu.make_async_copy(
                    received.at[pl.ds(g * shards, shards), pl.ds(k * block_len, block_len), :],
                    decode.at[0, g, :, :, pl.ds(k * rank, rank)],
                    sems.at[g, k],
                )
            )
    for c in copies:
        c.start()
    half = (rows - 2 * block_len) // 2
    for s in range(sources):
        g, x, y, c = s // 32, s // 8 % 4, s // 2 % 4, s % 2
        seq = 2 * x + y // 2
        part = received[s, 2 * block_len :, :].astype(jnp.float32)
        part = part[half:] + part[:half]
        first = g * 16 + c * 8 + y % 2 * 4
        for j in range(half):
            attended[seq : seq + 1, (first + j) * rank : (first + j + 1) * rank] = part[j : j + 1]
    for c in copies:
        c.wait()


def unpack(received, groups, batch, heads, block_len):
    sources, _, rank = received.shape
    return pl.pallas_call(
        unpack_kernel,
        out_shape=(
            jax.ShapeDtypeStruct(
                (1, groups, sources // groups, block_len, 2 * rank), received.dtype
            ),
            jax.ShapeDtypeStruct((batch, heads * rank), jnp.float32),
        ),
        in_specs=[VMEM],
        out_specs=(pl.BlockSpec(memory_space=pl.ANY), VMEM),
        scratch_shapes=[pltpu.SemaphoreType.DMA((groups, 2))],
        compiler_params=PARAMS,
        name="unpack",
    )(received)


def swap(x, axis, mask):
    return lax.ppermute(x, axis, [(i, i ^ mask) for i in range(lax.axis_size(axis))])


def body(latent, up_key, up_value, queries, lengths, block_dest):
    groups = up_key.shape[0]
    dests = latent.shape[1]
    block_len = latent.shape[2]
    batch, q_heads, _ = queries.shape
    table = lax.dynamic_slice_in_dim(block_dest, lax.axis_index(SEQ) * dests, dests)
    part = attend(latent[0], up_key, queries, lengths, q_heads // groups)
    part = merge(part, swap(part, "seq_2", 1))
    outgoing = pack(table, latent[0], part, swap(part, "seq_1", 1), up_value)
    received = lax.all_to_all(outgoing, GRP_SEQ, split_axis=0, concat_axis=0, tiled=True)
    return unpack(received, groups, batch, q_heads, block_len)


def solution(mesh):
    finer = Mesh(
        mesh.devices.reshape(mesh.shape["grp"], 4, 4, 2), ("grp", "seq_0", "seq_1", "seq_2")
    )
    in_specs = (P("grp", SEQ, None, None), P(), P(), P(), P(), P())
    out_specs = (P(GRP_SEQ, None, None, None, None), P())
    return jax.shard_map(body, mesh=finer, in_specs=in_specs, out_specs=out_specs, check_vma=False)
```

```python
import jax
import jax.numpy as jnp
from jax import lax
from jax.experimental import pallas as pl
from jax.experimental.pallas import tpu as pltpu
from jax.sharding import Mesh
from jax.sharding import PartitionSpec as P

SEQ = ("seq_0", "seq_1", "seq_2")
GRP_SEQ = ("grp", "seq_0", "seq_1", "seq_2")
NEG = -1e30
VMEM = pl.BlockSpec(memory_space=pltpu.VMEM)
HBM = pl.BlockSpec(memory_space=pltpu.HBM)
PARAMS = pltpu.CompilerParams(vmem_limit_bytes=16 << 20)


def split(x, parts):
    pieces = []
    for _ in range(parts):
        piece = x.astype(jnp.bfloat16).astype(jnp.float32)
        pieces.append(piece)
        x = x - piece
    return jnp.concatenate(pieces, axis=0).astype(jnp.bfloat16)


def attend_kernel(
    ends, dests, latent, up_key, queries, out, outgoing, lat, key_map, query, table, lengths, sems
):
    chunks, per_chunk, block_len, width = lat.shape
    rank = width // 2
    tokens = per_chunk * block_len
    heads, head_dim = query.shape
    per_group = key_map.shape[1] // head_dim
    per_kv = heads // per_group
    shard = lax.axis_index(SEQ)
    group = lax.axis_index("grp")
    quarter = lax.axis_size(SEQ) // queries.shape[0]
    seq = shard // quarter
    count = chunks * per_chunk
    small = [
        pltpu.make_async_copy(
            queries.at[seq, pl.ds(pl.multiple_of(group * heads, heads), heads)], query, sems.at[0]
        ),
        pltpu.make_async_copy(up_key.at[group], key_map, sems.at[1]),
        pltpu.make_async_copy(
            dests.at[pl.ds(pl.multiple_of(shard * count, count), count)], table, sems.at[2]
        ),
        pltpu.make_async_copy(ends, lengths, sems.at[3]),
    ]
    large = [
        pltpu.make_async_copy(latent.at[pl.ds(i * per_chunk, per_chunk)], lat.at[i], sems.at[4 + i])
        for i in range(chunks)
    ]
    for copy in small + large:
        copy.start()
    for copy in small:
        copy.wait()
    live_count = lengths[seq] - (shard % quarter) * (chunks * tokens)
    heads_f = query[...].astype(jnp.float32)
    rows = [
        lax.dot_general(
            heads_f[k * per_kv : (k + 1) * per_kv].astype(jnp.bfloat16),
            key_map[:, k * head_dim : (k + 1) * head_dim],
            (((1,), (1,)), ((), ())),
            preferred_element_type=jnp.float32,
        )
        for k in range(per_group)
    ]
    absorbed = split(jnp.concatenate(rows, axis=0) * (1.0 / float(head_dim) ** 0.5), 3)
    found = []
    for i in range(chunks):
        large[i].wait()
        both = lat[i].reshape(tokens, width)
        raw = lax.dot_general(
            absorbed,
            both[:, :rank],
            (((1,), (1,)), ((), ())),
            preferred_element_type=jnp.float32,
        )
        scores = raw[2 * heads :] + raw[heads : 2 * heads] + raw[:heads]
        position = lax.broadcasted_iota(jnp.int32, (heads, tokens), 1) + i * tokens
        live = position < live_count
        scores = jnp.where(live, scores, NEG)
        largest = jnp.max(scores, axis=1, keepdims=True)
        weights = jnp.where(live, jnp.exp(scores - largest), 0.0)
        total = jnp.sum(weights, axis=1, keepdims=True)
        summed = lax.dot_general(
            split(weights, 2),
            both[:, rank:],
            (((1,), (0,)), ((), ())),
            preferred_element_type=jnp.float32,
        )
        found.append((summed[:heads] + summed[heads:], largest, total))
        for j in range(per_chunk):
            to = table[i * per_chunk + j]
            outgoing[to, :block_len, :] = lat[i, j, :, :rank]
            outgoing[to, block_len : 2 * block_len, :] = lat[i, j, :, rank:]
    largest = found[0][1]
    for _, other, _ in found[1:]:
        largest = jnp.maximum(largest, other)
    factors = [jnp.exp(f[1] - largest) for f in found]
    out[0] = sum(f[0] * k for f, k in zip(found, factors))
    out[1] = jnp.broadcast_to(largest, (heads, rank))
    out[2] = jnp.broadcast_to(sum(f[2] * k for f, k in zip(found, factors)), (heads, rank))


def attend(latent, up_key, queries, lengths, block_dest, chunks, extra):
    count, block_len, width = latent.shape
    groups = up_key.shape[0]
    _, q_heads, head_dim = queries.shape
    heads = q_heads // groups
    rank = width // 2
    return pl.pallas_call(
        attend_kernel,
        out_shape=(
            jax.ShapeDtypeStruct((3, heads, rank), jnp.float32),
            jax.ShapeDtypeStruct((count, 2 * block_len + extra, rank), latent.dtype),
        ),
        in_specs=[HBM] * 5,
        out_specs=(VMEM, VMEM),
        scratch_shapes=[
            pltpu.VMEM((chunks, count // chunks, block_len, width), latent.dtype),
            pltpu.VMEM(up_key.shape[1:], up_key.dtype),
            pltpu.VMEM((heads, head_dim), queries.dtype),
            pltpu.SMEM((count,), jnp.int32),
            pltpu.SMEM(lengths.shape, jnp.int32),
            pltpu.SemaphoreType.DMA((4 + chunks,)),
        ],
        compiler_params=PARAMS,
        name="attend",
    )(lengths, block_dest, latent, up_key, queries)


def joined(first, second):
    largest = jnp.maximum(first[1], second[1])
    factor_a = jnp.exp(first[1] - largest)
    factor_b = jnp.exp(second[1] - largest)
    accum = first[0] * factor_a + second[0] * factor_b
    return (accum, largest, first[2] * factor_a + second[2] * factor_b)


def merge_kernel(mine, theirs, out):
    kept = out.shape[1]
    rows = pl.ds(pl.multiple_of(lax.axis_index("seq_2") * kept, kept), kept)
    both = joined(
        [mine[i, rows, :] for i in range(3)], [theirs[i, rows, :] for i in range(3)]
    )
    for i in range(3):
        out[i] = both[i]


def merge(mine, theirs):
    return pl.pallas_call(
        merge_kernel,
        out_shape=jax.ShapeDtypeStruct((3, mine.shape[1] // 2, mine.shape[2]), jnp.float32),
        in_specs=[VMEM, VMEM],
        out_specs=VMEM,
        compiler_params=PARAMS,
        name="merge",
    )(mine, theirs)


def pack_kernel(mine, theirs, up_value, _, out):
    head_dim = mine.shape[2]
    accum, _, total = joined([mine[i] for i in range(3)], [theirs[i] for i in range(3)])
    mean = accum / total
    half = mean.shape[0] // 2
    mean = jnp.where(lax.axis_index("seq_1") % 2 == 1, mean[half:], mean[:half])
    value_map = up_value[lax.axis_index("grp")]
    value_map = jnp.where(
        lax.axis_index("seq_2") == 1, value_map[:, head_dim:], value_map[:, :head_dim]
    )
    wide = lax.dot_general(
        split(mean, 3), value_map, (((1,), (0,)), ((), ())), preferred_element_type=jnp.float32
    )
    extra = split(wide[2 * half :] + wide[half : 2 * half] + wide[:half], 2)
    rows = out.shape[1] - extra.shape[0]
    for b in range(out.shape[0]):
        out[b, rows:, :] = extra


def pack(mine, theirs, up_value, outgoing):
    return pl.pallas_call(
        pack_kernel,
        out_shape=jax.ShapeDtypeStruct(outgoing.shape, outgoing.dtype),
        in_specs=[VMEM] * 4,
        out_specs=VMEM,
        input_output_aliases={3: 0},
        compiler_params=PARAMS,
        name="pack",
    )(mine, theirs, up_value, outgoing)


def unpack_kernel(received, decode, attended, rows_out, sems, row_sems):
    sources, rows, rank = received.shape
    _, groups, shards, block_len, _ = decode.shape
    copies = []
    for g in range(groups):
        for k in range(2):
            copies.append(
                pltpu.make_async_copy(
                    received.at[pl.ds(g * shards, shards), pl.ds(k * block_len, block_len), :],
                    decode.at[0, g, :, :, pl.ds(k * rank, rank)],
                    sems.at[g, k],
                )
            )
    for c in copies:
        c.start()
    half = (rows - 2 * block_len) // 2
    span = rows_out.shape[1] // groups
    for g in range(groups):
        for s in range(shards):
            x, y, c = s // 8, s // 2 % 4, s % 2
            seq = 2 * x + y // 2
            part = received[g * shards + s, 2 * block_len :, :].astype(jnp.float32)
            part = part[half:] + part[:half]
            first = g * 16 + c * 8 + y % 2 * 4
            for j in range(half):
                at = (first + j) * rank
                rows_out[seq : seq + 1, at : at + rank] = part[j : j + 1]
        columns = pl.ds(g * span, span)
        copy = pltpu.make_async_copy(
            rows_out.at[:, columns], attended.at[:, columns], row_sems.at[g]
        )
        copy.start()
        copies.append(copy)
    for c in copies:
        c.wait()


def unpack(received, groups, batch, heads, block_len):
    sources, _, rank = received.shape
    return pl.pallas_call(
        unpack_kernel,
        out_shape=(
            jax.ShapeDtypeStruct(
                (1, groups, sources // groups, block_len, 2 * rank), received.dtype
            ),
            jax.ShapeDtypeStruct((batch, heads * rank), jnp.float32),
        ),
        in_specs=[VMEM],
        out_specs=(HBM, HBM),
        scratch_shapes=[
            pltpu.VMEM((batch, heads * rank), jnp.float32),
            pltpu.SemaphoreType.DMA((groups, 2)),
            pltpu.SemaphoreType.DMA((groups,)),
        ],
        compiler_params=PARAMS,
        name="unpack",
    )(received)


def swap(x, axis, mask):
    return lax.ppermute(x, axis, [(i, i ^ mask) for i in range(lax.axis_size(axis))])


def body(latent, up_key, up_value, queries, lengths, block_dest):
    groups = up_key.shape[0]
    block_len = latent.shape[2]
    batch, q_heads, _ = queries.shape
    part, outgoing = attend(latent[0], up_key, queries, lengths, block_dest, 4, 8)
    part = merge(part, swap(part, "seq_2", 1))
    outgoing = pack(part, swap(part, "seq_1", 1), up_value, outgoing)
    received = lax.all_to_all(outgoing, GRP_SEQ, split_axis=0, concat_axis=0, tiled=True)
    return unpack(received, groups, batch, q_heads, block_len)


def solution(mesh):
    finer = Mesh(
        mesh.devices.reshape(mesh.shape["grp"], 4, 4, 2), ("grp", "seq_0", "seq_1", "seq_2")
    )
    in_specs = (P("grp", SEQ, None, None), P(), P(), P(), P(), P())
    out_specs = (P(GRP_SEQ, None, None, None, None), P())
    return jax.shard_map(body, mesh=finer, in_specs=in_specs, out_specs=out_specs, check_vma=False)
```

```python
import jax
import jax.numpy as jnp
from jax import lax
from jax.experimental import pallas as pl
from jax.experimental.pallas import tpu as pltpu
from jax.sharding import Mesh
from jax.sharding import PartitionSpec as P

SEQ = ("seq_0", "seq_1", "seq_2")
GRP_SEQ = ("grp", "seq_0", "seq_1", "seq_2")
NEG = -1e30
VMEM = pl.BlockSpec(memory_space=pltpu.VMEM)
HBM = pl.BlockSpec(memory_space=pltpu.HBM)
PARAMS = pltpu.CompilerParams(vmem_limit_bytes=16 << 20)


def split(x, parts):
    pieces = []
    for _ in range(parts):
        piece = x.astype(jnp.bfloat16).astype(jnp.float32)
        pieces.append(piece)
        x = x - piece
    return jnp.concatenate(pieces, axis=0).astype(jnp.bfloat16)


def attend_kernel(
    ends, dests, latent, up_key, queries, out, outgoing, lat, key_map, query, table, lengths, sems
):
    chunks, per_chunk, block_len, width = lat.shape
    rank = width // 2
    tokens = per_chunk * block_len
    heads, head_dim = query.shape
    per_group = key_map.shape[1] // head_dim
    per_kv = heads // per_group
    shard = lax.axis_index(SEQ)
    group = lax.axis_index("grp")
    quarter = lax.axis_size(SEQ) // queries.shape[0]
    seq = shard // quarter
    count = chunks * per_chunk
    small = [
        pltpu.make_async_copy(
            queries.at[seq, pl.ds(pl.multiple_of(group * heads, heads), heads)], query, sems.at[0]
        ),
        pltpu.make_async_copy(up_key.at[group], key_map, sems.at[1]),
        pltpu.make_async_copy(
            dests.at[pl.ds(pl.multiple_of(shard * count, count), count)], table, sems.at[2]
        ),
        pltpu.make_async_copy(ends, lengths, sems.at[3]),
    ]
    large = [
        pltpu.make_async_copy(latent.at[pl.ds(i * per_chunk, per_chunk)], lat.at[i], sems.at[4 + i])
        for i in range(chunks)
    ]
    for copy in small + large:
        copy.start()
    for copy in small:
        copy.wait()
    live_count = lengths[seq] - (shard % quarter) * (chunks * tokens)
    heads_f = query[...].astype(jnp.float32)
    rows = [
        lax.dot_general(
            heads_f[k * per_kv : (k + 1) * per_kv].astype(jnp.bfloat16),
            key_map[:, k * head_dim : (k + 1) * head_dim],
            (((1,), (1,)), ((), ())),
            preferred_element_type=jnp.float32,
        )
        for k in range(per_group)
    ]
    absorbed = split(jnp.concatenate(rows, axis=0) * (1.0 / float(head_dim) ** 0.5), 3)
    found = []
    for i in range(chunks):
        large[i].wait()
        both = lat[i].reshape(tokens, width)
        raw = lax.dot_general(
            absorbed,
            both[:, :rank],
            (((1,), (1,)), ((), ())),
            preferred_element_type=jnp.float32,
        )
        scores = raw[2 * heads :] + raw[heads : 2 * heads] + raw[:heads]
        position = lax.broadcasted_iota(jnp.int32, (heads, tokens), 1) + i * tokens
        live = position < live_count
        scores = jnp.where(live, scores, NEG)
        largest = jnp.max(scores, axis=1, keepdims=True)
        weights = jnp.where(live, jnp.exp(scores - largest), 0.0)
        total = jnp.sum(weights, axis=1, keepdims=True)
        summed = lax.dot_general(
            split(weights, 2),
            both[:, rank:],
            (((1,), (0,)), ((), ())),
            preferred_element_type=jnp.float32,
        )
        found.append((summed[:heads] + summed[heads:], largest, total))
        for j in range(per_chunk):
            to = table[i * per_chunk + j]
            outgoing[to, :block_len, :] = lat[i, j, :, :rank]
            outgoing[to, block_len : 2 * block_len, :] = lat[i, j, :, rank:]
    largest = found[0][1]
    for _, other, _ in found[1:]:
        largest = jnp.maximum(largest, other)
    factors = [jnp.exp(f[1] - largest) for f in found]
    out[0] = sum(f[0] * k for f, k in zip(found, factors))
    out[1] = jnp.broadcast_to(largest, (heads, rank))
    out[2] = jnp.broadcast_to(sum(f[2] * k for f, k in zip(found, factors)), (heads, rank))


def attend(latent, up_key, queries, lengths, block_dest, chunks, extra):
    count, block_len, width = latent.shape
    groups = up_key.shape[0]
    _, q_heads, head_dim = queries.shape
    heads = q_heads // groups
    rank = width // 2
    return pl.pallas_call(
        attend_kernel,
        out_shape=(
            jax.ShapeDtypeStruct((3, heads, rank), jnp.float32),
            jax.ShapeDtypeStruct((count, 2 * block_len + extra, rank), latent.dtype),
        ),
        in_specs=[HBM] * 5,
        out_specs=(VMEM, VMEM),
        scratch_shapes=[
            pltpu.VMEM((chunks, count // chunks, block_len, width), latent.dtype),
            pltpu.VMEM(up_key.shape[1:], up_key.dtype),
            pltpu.VMEM((heads, head_dim), queries.dtype),
            pltpu.SMEM((count,), jnp.int32),
            pltpu.SMEM(lengths.shape, jnp.int32),
            pltpu.SemaphoreType.DMA((4 + chunks,)),
        ],
        compiler_params=PARAMS,
        name="attend",
    )(*[
        pltpu.with_memory_space_constraint(x, pltpu.HBM)
        for x in (lengths, block_dest, latent, up_key, queries)
    ])


def joined(first, second):
    largest = jnp.maximum(first[1], second[1])
    factor_a = jnp.exp(first[1] - largest)
    factor_b = jnp.exp(second[1] - largest)
    accum = first[0] * factor_a + second[0] * factor_b
    return (accum, largest, first[2] * factor_a + second[2] * factor_b)


def merge_kernel(mine, theirs, out):
    kept = out.shape[1]
    rows = pl.ds(pl.multiple_of(lax.axis_index("seq_2") * kept, kept), kept)
    both = joined(
        [mine[i, rows, :] for i in range(3)], [theirs[i, rows, :] for i in range(3)]
    )
    for i in range(3):
        out[i] = both[i]


def merge(mine, theirs):
    return pl.pallas_call(
        merge_kernel,
        out_shape=jax.ShapeDtypeStruct((3, mine.shape[1] // 2, mine.shape[2]), jnp.float32),
        in_specs=[VMEM, VMEM],
        out_specs=VMEM,
        compiler_params=PARAMS,
        name="merge",
    )(mine, theirs)


def pack_kernel(mine, theirs, up_value, _, out):
    head_dim = mine.shape[2]
    accum, _, total = joined([mine[i] for i in range(3)], [theirs[i] for i in range(3)])
    mean = accum / total
    half = mean.shape[0] // 2
    mean = jnp.where(lax.axis_index("seq_1") % 2 == 1, mean[half:], mean[:half])
    value_map = up_value[lax.axis_index("grp")]
    value_map = jnp.where(
        lax.axis_index("seq_2") == 1, value_map[:, head_dim:], value_map[:, :head_dim]
    )
    wide = lax.dot_general(
        split(mean, 3), value_map, (((1,), (0,)), ((), ())), preferred_element_type=jnp.float32
    )
    extra = split(wide[2 * half :] + wide[half : 2 * half] + wide[:half], 2)
    rows = out.shape[1] - extra.shape[0]
    for b in range(out.shape[0]):
        out[b, rows:, :] = extra


def pack(mine, theirs, up_value, outgoing):
    return pl.pallas_call(
        pack_kernel,
        out_shape=jax.ShapeDtypeStruct(outgoing.shape, outgoing.dtype),
        in_specs=[VMEM] * 4,
        out_specs=VMEM,
        input_output_aliases={3: 0},
        compiler_params=PARAMS,
        name="pack",
    )(mine, theirs, up_value, outgoing)


def unpack_kernel(received, decode, attended, rows_out, sems, row_sems):
    sources, rows, rank = received.shape
    _, groups, shards, block_len, _ = decode.shape
    copies = []
    for g in range(groups):
        for k in range(2):
            copies.append(
                pltpu.make_async_copy(
                    received.at[pl.ds(g * shards, shards), pl.ds(k * block_len, block_len), :],
                    decode.at[0, g, :, :, pl.ds(k * rank, rank)],
                    sems.at[g, k],
                )
            )
    for c in copies:
        c.start()
    half = (rows - 2 * block_len) // 2
    span = rows_out.shape[1] // groups
    for g in range(groups):
        for s in range(shards):
            x, y, c = s // 8, s // 2 % 4, s % 2
            seq = 2 * x + y // 2
            part = received[g * shards + s, 2 * block_len :, :].astype(jnp.float32)
            part = part[half:] + part[:half]
            first = g * 16 + c * 8 + y % 2 * 4
            for j in range(half):
                at = (first + j) * rank
                rows_out[seq : seq + 1, at : at + rank] = part[j : j + 1]
        columns = pl.ds(g * span, span)
        copy = pltpu.make_async_copy(
            rows_out.at[:, columns], attended.at[:, columns], row_sems.at[g]
        )
        copy.start()
        copies.append(copy)
    for c in copies:
        c.wait()


def unpack(received, groups, batch, heads, block_len):
    sources, _, rank = received.shape
    return pl.pallas_call(
        unpack_kernel,
        out_shape=(
            jax.ShapeDtypeStruct(
                (1, groups, sources // groups, block_len, 2 * rank), received.dtype
            ),
            jax.ShapeDtypeStruct((batch, heads * rank), jnp.float32),
        ),
        in_specs=[VMEM],
        out_specs=(HBM, HBM),
        scratch_shapes=[
            pltpu.VMEM((batch, heads * rank), jnp.float32),
            pltpu.SemaphoreType.DMA((groups, 2)),
            pltpu.SemaphoreType.DMA((groups,)),
        ],
        compiler_params=PARAMS,
        name="unpack",
    )(received)


def swap(x, axis, mask):
    return lax.ppermute(x, axis, [(i, i ^ mask) for i in range(lax.axis_size(axis))])


def body(latent, up_key, up_value, queries, lengths, block_dest):
    groups = up_key.shape[0]
    block_len = latent.shape[2]
    batch, q_heads, _ = queries.shape
    part, outgoing = attend(latent[0], up_key, queries, lengths, block_dest, 4, 8)
    part = merge(part, swap(part, "seq_2", 1))
    outgoing = pack(part, swap(part, "seq_1", 1), up_value, outgoing)
    received = lax.all_to_all(outgoing, GRP_SEQ, split_axis=0, concat_axis=0, tiled=True)
    return unpack(received, groups, batch, q_heads, block_len)


def solution(mesh):
    finer = Mesh(
        mesh.devices.reshape(mesh.shape["grp"], 4, 4, 2), ("grp", "seq_0", "seq_1", "seq_2")
    )
    in_specs = (P("grp", SEQ, None, None), P(), P(), P(), P(), P())
    out_specs = (P(GRP_SEQ, None, None, None, None), P())
    return jax.shard_map(body, mesh=finer, in_specs=in_specs, out_specs=out_specs, check_vma=False)
```

```python
import jax
import jax.numpy as jnp
from jax import lax
from jax.experimental import pallas as pl
from jax.experimental.pallas import tpu as pltpu
from jax.sharding import Mesh
from jax.sharding import PartitionSpec as P

SEQ = ("seq_0", "seq_1", "seq_2")
GRP_SEQ = ("grp", "seq_0", "seq_1", "seq_2")
NEG = -1e30
VMEM = pl.BlockSpec(memory_space=pltpu.VMEM)
HBM = pl.BlockSpec(memory_space=pltpu.HBM)
PARAMS = pltpu.CompilerParams(vmem_limit_bytes=16 << 20)


def split(x, parts):
    pieces = []
    for _ in range(parts):
        piece = x.astype(jnp.bfloat16).astype(jnp.float32)
        pieces.append(piece)
        x = x - piece
    return jnp.concatenate(pieces, axis=0).astype(jnp.bfloat16)


def attend_kernel(
    ends, latent, up_key, queries, out, key, value, key_map, query, lengths, sems
):
    count, block_len, rank = key.shape
    tokens = count * block_len
    heads, head_dim = query.shape
    per_group = key_map.shape[1] // head_dim
    per_kv = heads // per_group
    shard = lax.axis_index(SEQ)
    group = lax.axis_index("grp")
    quarter = lax.axis_size(SEQ) // queries.shape[0]
    seq = shard // quarter
    first = pl.multiple_of(group * heads, heads)
    copies = [
        pltpu.make_async_copy(queries.at[seq, pl.ds(first, heads)], query, sems.at[0]),
        pltpu.make_async_copy(up_key.at[group], key_map, sems.at[1]),
        pltpu.make_async_copy(ends, lengths, sems.at[2]),
        pltpu.make_async_copy(latent.at[:, :, pl.ds(0, rank)], key, sems.at[3]),
        pltpu.make_async_copy(latent.at[:, :, pl.ds(rank, rank)], value, sems.at[4]),
    ]
    for copy in copies:
        copy.start()
    for copy in copies[:3]:
        copy.wait()
    live_count = lengths[seq] - (shard % quarter) * tokens
    heads_f = query[...].astype(jnp.float32)
    rows = [
        lax.dot_general(
            heads_f[k * per_kv : (k + 1) * per_kv].astype(jnp.bfloat16),
            key_map[:, k * head_dim : (k + 1) * head_dim],
            (((1,), (1,)), ((), ())),
            preferred_element_type=jnp.float32,
        )
        for k in range(per_group)
    ]
    absorbed = split(jnp.concatenate(rows, axis=0) * (1.0 / float(head_dim) ** 0.5), 3)
    copies[3].wait()
    raw = lax.dot_general(
        absorbed,
        key[...].reshape(tokens, rank),
        (((1,), (1,)), ((), ())),
        preferred_element_type=jnp.float32,
    )
    scores = raw[2 * heads :] + raw[heads : 2 * heads] + raw[:heads]
    live = lax.broadcasted_iota(jnp.int32, (heads, tokens), 1) < live_count
    scores = jnp.where(live, scores, NEG)
    largest = jnp.max(scores, axis=1, keepdims=True)
    weights = jnp.where(live, jnp.exp(scores - largest), 0.0)
    total = jnp.sum(weights, axis=1, keepdims=True)
    halves = split(weights, 2)
    copies[4].wait()
    summed = lax.dot_general(
        halves,
        value[...].reshape(tokens, rank),
        (((1,), (0,)), ((), ())),
        preferred_element_type=jnp.float32,
    )
    out[0] = summed[:heads] + summed[heads:]
    out[1] = jnp.broadcast_to(largest, (heads, rank))
    out[2] = jnp.broadcast_to(total, (heads, rank))


def attend(latent, up_key, queries, lengths):
    count, block_len, width = latent.shape
    heads = queries.shape[1] // up_key.shape[0]
    rank = width // 2
    return pl.pallas_call(
        attend_kernel,
        out_shape=(
            jax.ShapeDtypeStruct((3, heads, rank), jnp.float32),
            jax.ShapeDtypeStruct((count, block_len, rank), latent.dtype),
            jax.ShapeDtypeStruct((count, block_len, rank), latent.dtype),
        ),
        in_specs=[HBM] * 4,
        out_specs=(VMEM,) * 3,
        scratch_shapes=[
            pltpu.VMEM(up_key.shape[1:], up_key.dtype),
            pltpu.VMEM((heads, queries.shape[2]), queries.dtype),
            pltpu.SMEM(lengths.shape, jnp.int32),
            pltpu.SemaphoreType.DMA((5,)),
        ],
        compiler_params=PARAMS,
        name="attend",
    )(*[in_hbm(x) for x in (lengths, latent, up_key, queries)])


def in_hbm(x):
    return pltpu.with_memory_space_constraint(x, pltpu.HBM)


def slot_kernel(dests, key, value, after, outgoing, table, sem):
    count, block_len, _ = key.shape
    first = pl.multiple_of(lax.axis_index(SEQ) * count, count)
    copy = pltpu.make_async_copy(dests.at[pl.ds(first, count)], table, sem)
    copy.start()
    copy.wait()
    for b in range(count):
        to = table[b]
        outgoing[to, :block_len, :] = key[b]
        outgoing[to, block_len : 2 * block_len, :] = value[b]


def slot(block_dest, key, value, after, extra):
    count, block_len, rank = key.shape
    return pl.pallas_call(
        slot_kernel,
        out_shape=jax.ShapeDtypeStruct((count, 2 * block_len + extra, rank), key.dtype),
        in_specs=[HBM, VMEM, VMEM, VMEM],
        out_specs=VMEM,
        scratch_shapes=[pltpu.SMEM((count,), jnp.int32), pltpu.SemaphoreType.DMA],
        compiler_params=PARAMS,
        name="slot",
    )(in_hbm(block_dest), key, value, after)


def joined(first, second):
    largest = jnp.maximum(first[1], second[1])
    factor_a = jnp.exp(first[1] - largest)
    factor_b = jnp.exp(second[1] - largest)
    accum = first[0] * factor_a + second[0] * factor_b
    return (accum, largest, first[2] * factor_a + second[2] * factor_b)


def merge_kernel(mine, theirs, out):
    kept = out.shape[1]
    rows = pl.ds(pl.multiple_of(lax.axis_index("seq_2") * kept, kept), kept)
    both = joined(
        [mine[i, rows, :] for i in range(3)], [theirs[i, rows, :] for i in range(3)]
    )
    for i in range(3):
        out[i] = both[i]


def merge(mine, theirs):
    return pl.pallas_call(
        merge_kernel,
        out_shape=jax.ShapeDtypeStruct((3, mine.shape[1] // 2, mine.shape[2]), jnp.float32),
        in_specs=[VMEM, VMEM],
        out_specs=VMEM,
        compiler_params=PARAMS,
        name="merge",
    )(mine, theirs)


def pack_kernel(mine, theirs, up_value, _, out):
    head_dim = mine.shape[2]
    accum, _, total = joined([mine[i] for i in range(3)], [theirs[i] for i in range(3)])
    mean = accum / total
    half = mean.shape[0] // 2
    mean = jnp.where(lax.axis_index("seq_1") % 2 == 1, mean[half:], mean[:half])
    value_map = up_value[lax.axis_index("grp")]
    value_map = jnp.where(
        lax.axis_index("seq_2") == 1, value_map[:, head_dim:], value_map[:, :head_dim]
    )
    wide = lax.dot_general(
        split(mean, 3), value_map, (((1,), (0,)), ((), ())), preferred_element_type=jnp.float32
    )
    extra = split(wide[2 * half :] + wide[half : 2 * half] + wide[:half], 2)
    rows = out.shape[1] - extra.shape[0]
    for b in range(out.shape[0]):
        out[b, rows:, :] = extra


def pack(mine, theirs, up_value, outgoing):
    return pl.pallas_call(
        pack_kernel,
        out_shape=jax.ShapeDtypeStruct(outgoing.shape, outgoing.dtype),
        in_specs=[VMEM] * 4,
        out_specs=VMEM,
        input_output_aliases={3: 0},
        compiler_params=PARAMS,
        name="pack",
    )(mine, theirs, up_value, outgoing)


def unpack_kernel(received, decode, attended, rows_out, sems, row_sems):
    sources, rows, rank = received.shape
    _, groups, shards, block_len, _ = decode.shape
    copies = []
    for g in range(groups):
        for k in range(2):
            copies.append(
                pltpu.make_async_copy(
                    received.at[pl.ds(g * shards, shards), pl.ds(k * block_len, block_len), :],
                    decode.at[0, g, :, :, pl.ds(k * rank, rank)],
                    sems.at[g, k],
                )
            )
    for c in copies:
        c.start()
    half = (rows - 2 * block_len) // 2
    span = rows_out.shape[1] // groups
    for g in range(groups):
        for s in range(shards):
            x, y, c = s // 8, s // 2 % 4, s % 2
            seq = 2 * x + y // 2
            part = received[g * shards + s, 2 * block_len :, :].astype(jnp.float32)
            part = part[half:] + part[:half]
            first = g * 16 + c * 8 + y % 2 * 4
            for j in range(half):
                at = (first + j) * rank
                rows_out[seq : seq + 1, at : at + rank] = part[j : j + 1]
        columns = pl.ds(g * span, span)
        copy = pltpu.make_async_copy(
            rows_out.at[:, columns], attended.at[:, columns], row_sems.at[g]
        )
        copy.start()
        copies.append(copy)
    for c in copies:
        c.wait()


def unpack(received, groups, batch, heads, block_len):
    sources, _, rank = received.shape
    return pl.pallas_call(
        unpack_kernel,
        out_shape=(
            jax.ShapeDtypeStruct(
                (1, groups, sources // groups, block_len, 2 * rank), received.dtype
            ),
            jax.ShapeDtypeStruct((batch, heads * rank), jnp.float32),
        ),
        in_specs=[VMEM],
        out_specs=(HBM, HBM),
        scratch_shapes=[
            pltpu.VMEM((batch, heads * rank), jnp.float32),
            pltpu.SemaphoreType.DMA((groups, 2)),
            pltpu.SemaphoreType.DMA((groups,)),
        ],
        compiler_params=PARAMS,
        name="unpack",
    )(received)


def swap(x, axis, mask):
    return lax.ppermute(x, axis, [(i, i ^ mask) for i in range(lax.axis_size(axis))])


def body(latent, up_key, up_value, queries, lengths, block_dest):
    groups = up_key.shape[0]
    block_len = latent.shape[2]
    batch, q_heads, _ = queries.shape
    part, key, value = attend(latent[0], up_key, queries, lengths)
    part = merge(part, swap(part, "seq_2", 1))
    outgoing = slot(block_dest, key, value, part, 8)
    outgoing = pack(part, swap(part, "seq_1", 1), up_value, outgoing)
    received = lax.all_to_all(outgoing, GRP_SEQ, split_axis=0, concat_axis=0, tiled=True)
    return unpack(received, groups, batch, q_heads, block_len)


def solution(mesh):
    finer = Mesh(
        mesh.devices.reshape(mesh.shape["grp"], 4, 4, 2), ("grp", "seq_0", "seq_1", "seq_2")
    )
    in_specs = (P("grp", SEQ, None, None), P(), P(), P(), P(), P())
    out_specs = (P(GRP_SEQ, None, None, None, None), P())
    return jax.shard_map(body, mesh=finer, in_specs=in_specs, out_specs=out_specs, check_vma=False)
```

```python
import jax
import jax.numpy as jnp
from jax import lax
from jax.experimental import pallas as pl
from jax.experimental.pallas import tpu as pltpu
from jax.sharding import Mesh
from jax.sharding import PartitionSpec as P

SEQ = ("seq_0", "seq_1", "seq_2")
GRP_SEQ = ("grp", "seq_0", "seq_1", "seq_2")
NEG = -1e30
VMEM = pl.BlockSpec(memory_space=pltpu.VMEM)
HBM = pl.BlockSpec(memory_space=pltpu.HBM)
PARAMS = pltpu.CompilerParams(vmem_limit_bytes=16 << 20)


def split(x, parts):
    pieces = []
    for _ in range(parts):
        piece = x.astype(jnp.bfloat16).astype(jnp.float32)
        pieces.append(piece)
        x = x - piece
    return jnp.concatenate(pieces, axis=0).astype(jnp.bfloat16)


def attend_kernel(ends, latent, up_key, queries, out, lat, key_map, query, lengths, sems):
    count, block_len, width = lat.shape
    chunks = sems.shape[0] - 3
    blocks = count // chunks
    tokens = blocks * block_len
    rank = width // 2
    heads, head_dim = query.shape
    per_group = key_map.shape[1] // head_dim
    per_kv = heads // per_group
    shard = lax.axis_index(SEQ)
    group = lax.axis_index("grp")
    quarter = lax.axis_size(SEQ) // queries.shape[0]
    seq = shard // quarter
    first = pl.multiple_of(group * heads, heads)
    small = [
        pltpu.make_async_copy(queries.at[seq, pl.ds(first, heads)], query, sems.at[0]),
        pltpu.make_async_copy(up_key.at[group], key_map, sems.at[1]),
        pltpu.make_async_copy(ends, lengths, sems.at[2]),
    ]
    parts = [pl.ds(i * blocks, blocks) for i in range(chunks)]
    large = [
        pltpu.make_async_copy(latent.at[part], lat.at[part], sems.at[3 + i])
        for i, part in enumerate(parts)
    ]
    for copy in small + large:
        copy.start()
    for copy in small:
        copy.wait()
    live_count = lengths[seq] - (shard % quarter) * (count * block_len)
    heads_f = query[...].astype(jnp.float32)
    rows = [
        lax.dot_general(
            heads_f[k * per_kv : (k + 1) * per_kv].astype(jnp.bfloat16),
            key_map[:, k * head_dim : (k + 1) * head_dim],
            (((1,), (1,)), ((), ())),
            preferred_element_type=jnp.float32,
        )
        for k in range(per_group)
    ]
    absorbed = split(jnp.concatenate(rows, axis=0) * (1.0 / float(head_dim) ** 0.5), 3)

    def scored(i):
        raw = lax.dot_general(
            absorbed,
            lat[parts[i], :, :rank].reshape(tokens, rank),
            (((1,), (1,)), ((), ())),
            preferred_element_type=jnp.float32,
        )
        scores = raw[2 * heads :] + raw[heads : 2 * heads] + raw[:heads]
        position = lax.broadcasted_iota(jnp.int32, (heads, tokens), 1) + i * tokens
        live = position < live_count
        return (jnp.where(live, scores, NEG), live)

    def weighed(scores, live):
        largest = jnp.max(scores, axis=1, keepdims=True)
        weights = jnp.where(live, jnp.exp(scores - largest), 0.0)
        return (split(weights, 2), largest, jnp.sum(weights, axis=1, keepdims=True))

    def summed(i, halves, largest, total):
        both = lax.dot_general(
            halves,
            lat[parts[i], :, rank:].reshape(tokens, rank),
            (((1,), (0,)), ((), ())),
            preferred_element_type=jnp.float32,
        )
        return (both[:heads] + both[heads:], largest, total)

    scores, weights, found = ({}, {}, [])
    for step in range(chunks + 2):
        if step < chunks:
            large[step].wait()
            scores[step] = scored(step)
        if 0 <= step - 1 < chunks:
            weights[step - 1] = weighed(*scores.pop(step - 1))
        if step >= 2:
            found.append(summed(step - 2, *weights.pop(step - 2)))
    largest = found[0][1]
    for chunk in found[1:]:
        largest = jnp.maximum(largest, chunk[1])
    factors = [jnp.exp(f[1] - largest) for f in found]
    out[0] = sum(f[0] * k for f, k in zip(found, factors))
    out[1] = jnp.broadcast_to(largest, (heads, rank))
    out[2] = jnp.broadcast_to(sum(f[2] * k for f, k in zip(found, factors)), (heads, rank))


def attend(latent, up_key, queries, lengths, chunks):
    heads = queries.shape[1] // up_key.shape[0]
    return pl.pallas_call(
        attend_kernel,
        out_shape=(
            jax.ShapeDtypeStruct((3, heads, latent.shape[2] // 2), jnp.float32),
            jax.ShapeDtypeStruct(latent.shape, latent.dtype),
        ),
        in_specs=[HBM] * 4,
        out_specs=(VMEM,) * 2,
        scratch_shapes=[
            pltpu.VMEM(up_key.shape[1:], up_key.dtype),
            pltpu.VMEM((heads, queries.shape[2]), queries.dtype),
            pltpu.SMEM(lengths.shape, jnp.int32),
            pltpu.SemaphoreType.DMA((3 + chunks,)),
        ],
        compiler_params=PARAMS,
        name="attend",
    )(*[in_hbm(x) for x in (lengths, latent, up_key, queries)])


def in_hbm(x):
    return pltpu.with_memory_space_constraint(x, pltpu.HBM)


def slot_kernel(dests, lat, after, outgoing, table, sem):
    count, block_len, width = lat.shape
    rank = width // 2
    first = pl.multiple_of(lax.axis_index(SEQ) * count, count)
    copy = pltpu.make_async_copy(dests.at[pl.ds(first, count)], table, sem)
    copy.start()
    copy.wait()
    for b in range(count):
        to = table[b]
        outgoing[to, :block_len, :] = lat[b, :, :rank]
        outgoing[to, block_len : 2 * block_len, :] = lat[b, :, rank:]


def slot(block_dest, lat, after, extra):
    count, block_len, width = lat.shape
    return pl.pallas_call(
        slot_kernel,
        out_shape=jax.ShapeDtypeStruct((count, 2 * block_len + extra, width // 2), lat.dtype),
        in_specs=[HBM, VMEM, VMEM],
        out_specs=VMEM,
        scratch_shapes=[pltpu.SMEM((count,), jnp.int32), pltpu.SemaphoreType.DMA],
        compiler_params=PARAMS,
        name="slot",
    )(in_hbm(block_dest), lat, after)


def joined(first, second):
    largest = jnp.maximum(first[1], second[1])
    factor_a = jnp.exp(first[1] - largest)
    factor_b = jnp.exp(second[1] - largest)
    accum = first[0] * factor_a + second[0] * factor_b
    return (accum, largest, first[2] * factor_a + second[2] * factor_b)


def half_kept():
    return (lax.axis_index("seq_2") + lax.axis_index("seq_1")) % 2


def merge_kernel(mine, theirs, out):
    kept = out.shape[1]
    rows = pl.ds(pl.multiple_of(half_kept() * kept, kept), kept)
    both = joined(
        [mine[i, rows, :] for i in range(3)], [theirs[i, rows, :] for i in range(3)]
    )
    for i in range(3):
        out[i] = both[i]


def merge(mine, theirs):
    return pl.pallas_call(
        merge_kernel,
        out_shape=jax.ShapeDtypeStruct((3, mine.shape[1] // 2, mine.shape[2]), jnp.float32),
        in_specs=[VMEM, VMEM],
        out_specs=VMEM,
        compiler_params=PARAMS,
        name="merge",
    )(mine, theirs)


def pack_kernel(mine, theirs, up_value, _, out):
    head_dim = mine.shape[2]
    accum, _, total = joined([mine[i] for i in range(3)], [theirs[i] for i in range(3)])
    mean = accum / total
    half = mean.shape[0] // 2
    mean = jnp.where(lax.axis_index("seq_1") % 2 == 1, mean[half:], mean[:half])
    value_map = up_value[lax.axis_index("grp")]
    value_map = jnp.where(
        half_kept() == 1, value_map[:, head_dim:], value_map[:, :head_dim]
    )
    wide = lax.dot_general(
        split(mean, 3), value_map, (((1,), (0,)), ((), ())), preferred_element_type=jnp.float32
    )
    extra = split(wide[2 * half :] + wide[half : 2 * half] + wide[:half], 2)
    rows = out.shape[1] - extra.shape[0]
    for b in range(out.shape[0]):
        out[b, rows:, :] = extra


def pack(mine, theirs, up_value, outgoing):
    return pl.pallas_call(
        pack_kernel,
        out_shape=jax.ShapeDtypeStruct(outgoing.shape, outgoing.dtype),
        in_specs=[VMEM] * 4,
        out_specs=VMEM,
        input_output_aliases={3: 0},
        compiler_params=PARAMS,
        name="pack",
    )(mine, theirs, up_value, outgoing)


def unpack_kernel(received, decode, attended, rows_out, sems, row_sems):
    sources, rows, rank = received.shape
    _, groups, shards, block_len, _ = decode.shape
    copies = []
    for g in range(groups):
        for k in range(2):
            copies.append(
                pltpu.make_async_copy(
                    received.at[pl.ds(g * shards, shards), pl.ds(k * block_len, block_len), :],
                    decode.at[0, g, :, :, pl.ds(k * rank, rank)],
                    sems.at[g, k],
                )
            )
    for c in copies:
        c.start()
    half = (rows - 2 * block_len) // 2
    span = rows_out.shape[1] // groups
    for g in range(groups):
        for s in range(shards):
            x, y, c = s // 8, s // 2 % 4, s % 2
            seq = 2 * x + y // 2
            part = received[g * shards + s, 2 * block_len :, :].astype(jnp.float32)
            part = part[half:] + part[:half]
            first = g * 16 + (c + y) % 2 * 8 + y % 2 * 4
            for j in range(half):
                at = (first + j) * rank
                rows_out[seq : seq + 1, at : at + rank] = part[j : j + 1]
        columns = pl.ds(g * span, span)
        copy = pltpu.make_async_copy(
            rows_out.at[:, columns], attended.at[:, columns], row_sems.at[g]
        )
        copy.start()
        copies.append(copy)
    for c in copies:
        c.wait()


def unpack(received, groups, batch, heads, block_len):
    sources, _, rank = received.shape
    return pl.pallas_call(
        unpack_kernel,
        out_shape=(
            jax.ShapeDtypeStruct(
                (1, groups, sources // groups, block_len, 2 * rank), received.dtype
            ),
            jax.ShapeDtypeStruct((batch, heads * rank), jnp.float32),
        ),
        in_specs=[VMEM],
        out_specs=(HBM, HBM),
        scratch_shapes=[
            pltpu.VMEM((batch, heads * rank), jnp.float32),
            pltpu.SemaphoreType.DMA((groups, 2)),
            pltpu.SemaphoreType.DMA((groups,)),
        ],
        compiler_params=PARAMS,
        name="unpack",
    )(received)


def swap(x, axes, mask):
    return lax.ppermute(x, axes, [(i, i ^ mask) for i in range(lax.axis_size(axes))])


def body(latent, up_key, up_value, queries, lengths, block_dest):
    groups = up_key.shape[0]
    block_len = latent.shape[2]
    batch, q_heads, _ = queries.shape
    part, lat = attend(latent[0], up_key, queries, lengths, 2)
    part = merge(part, swap(part, "seq_2", 1))
    outgoing = slot(block_dest, lat, part, 8)
    outgoing = pack(part, swap(part, ("seq_1", "seq_2"), 3), up_value, outgoing)
    received = lax.all_to_all(outgoing, GRP_SEQ, split_axis=0, concat_axis=0, tiled=True)
    return unpack(received, groups, batch, q_heads, block_len)


def solution(mesh):
    finer = Mesh(
        mesh.devices.reshape(mesh.shape["grp"], 4, 4, 2), ("grp", "seq_0", "seq_1", "seq_2")
    )
    in_specs = (P("grp", SEQ, None, None), P(), P(), P(), P(), P())
    out_specs = (P(GRP_SEQ, None, None, None, None), P())
    return jax.shard_map(body, mesh=finer, in_specs=in_specs, out_specs=out_specs, check_vma=False)
```

```python
import jax
import jax.numpy as jnp
from jax import lax
from jax.experimental import pallas as pl
from jax.experimental.pallas import tpu as pltpu
from jax.sharding import Mesh
from jax.sharding import PartitionSpec as P

SEQ = ("seq_0", "seq_1", "seq_2")
GRP_SEQ = ("grp", "seq_0", "seq_1", "seq_2")
EXCHANGE = ("seq_2", "grp", "seq_0", "seq_1")
NEG = -1e30
VMEM = pl.BlockSpec(memory_space=pltpu.VMEM)
HBM = pl.BlockSpec(memory_space=pltpu.HBM)
PARAMS = pltpu.CompilerParams(vmem_limit_bytes=16 << 20)


def split(x, parts):
    pieces = []
    for _ in range(parts):
        piece = x.astype(jnp.bfloat16).astype(jnp.float32)
        pieces.append(piece)
        x = x - piece
    return jnp.concatenate(pieces, axis=0).astype(jnp.bfloat16)


def attend_kernel(ends, latent, up_key, queries, out, lat, key_map, query, lengths, sems):
    count, block_len, width = lat.shape
    chunks = sems.shape[0] - 3
    blocks = count // chunks
    tokens = blocks * block_len
    rank = width // 2
    heads, head_dim = query.shape
    per_group = key_map.shape[1] // head_dim
    per_kv = heads // per_group
    shard = lax.axis_index(SEQ)
    group = lax.axis_index("grp")
    quarter = lax.axis_size(SEQ) // queries.shape[0]
    seq = shard // quarter
    first = pl.multiple_of(group * heads, heads)
    small = [
        pltpu.make_async_copy(queries.at[seq, pl.ds(first, heads)], query, sems.at[0]),
        pltpu.make_async_copy(up_key.at[group], key_map, sems.at[1]),
        pltpu.make_async_copy(ends, lengths, sems.at[2]),
    ]
    parts = [pl.ds(i * blocks, blocks) for i in range(chunks)]
    large = [
        pltpu.make_async_copy(latent.at[part], lat.at[part], sems.at[3 + i])
        for i, part in enumerate(parts)
    ]
    for copy in small + large:
        copy.start()
    for copy in small:
        copy.wait()
    live_count = lengths[seq] - (shard % quarter) * (count * block_len)
    heads_f = query[...].astype(jnp.float32)
    rows = [
        lax.dot_general(
            heads_f[k * per_kv : (k + 1) * per_kv].astype(jnp.bfloat16),
            key_map[:, k * head_dim : (k + 1) * head_dim],
            (((1,), (1,)), ((), ())),
            preferred_element_type=jnp.float32,
        )
        for k in range(per_group)
    ]
    absorbed = split(jnp.concatenate(rows, axis=0) * (1.0 / float(head_dim) ** 0.5), 3)

    def scored(i):
        raw = lax.dot_general(
            absorbed,
            lat[parts[i], :, :rank].reshape(tokens, rank),
            (((1,), (1,)), ((), ())),
            preferred_element_type=jnp.float32,
        )
        scores = raw[2 * heads :] + raw[heads : 2 * heads] + raw[:heads]
        position = lax.broadcasted_iota(jnp.int32, (heads, tokens), 1) + i * tokens
        live = position < live_count
        return (jnp.where(live, scores, NEG), live)

    def weighed(scores, live):
        largest = jnp.max(scores, axis=1, keepdims=True)
        weights = jnp.where(live, jnp.exp(scores - largest), 0.0)
        return (split(weights, 2), largest, jnp.sum(weights, axis=1, keepdims=True))

    def summed(i, halves, largest, total):
        both = lax.dot_general(
            halves,
            lat[parts[i], :, rank:].reshape(tokens, rank),
            (((1,), (0,)), ((), ())),
            preferred_element_type=jnp.float32,
        )
        return (both[:heads] + both[heads:], largest, total)

    scores, weights, found = ({}, {}, [])
    for step in range(chunks + 2):
        if step < chunks:
            large[step].wait()
            scores[step] = scored(step)
        if 0 <= step - 1 < chunks:
            weights[step - 1] = weighed(*scores.pop(step - 1))
        if step >= 2:
            found.append(summed(step - 2, *weights.pop(step - 2)))
    largest = found[0][1]
    for chunk in found[1:]:
        largest = jnp.maximum(largest, chunk[1])
    factors = [jnp.exp(f[1] - largest) for f in found]
    out[0] = sum(f[0] * k for f, k in zip(found, factors))
    out[1] = jnp.broadcast_to(largest, (heads, rank))
    out[2] = jnp.broadcast_to(sum(f[2] * k for f, k in zip(found, factors)), (heads, rank))


def attend(latent, up_key, queries, lengths, chunks):
    heads = queries.shape[1] // up_key.shape[0]
    return pl.pallas_call(
        attend_kernel,
        out_shape=(
            jax.ShapeDtypeStruct((3, heads, latent.shape[2] // 2), jnp.float32),
            jax.ShapeDtypeStruct(latent.shape, latent.dtype),
        ),
        in_specs=[HBM] * 4,
        out_specs=(VMEM,) * 2,
        scratch_shapes=[
            pltpu.VMEM(up_key.shape[1:], up_key.dtype),
            pltpu.VMEM((heads, queries.shape[2]), queries.dtype),
            pltpu.SMEM(lengths.shape, jnp.int32),
            pltpu.SemaphoreType.DMA((3 + chunks,)),
        ],
        compiler_params=PARAMS,
        name="attend",
    )(*[in_hbm(x) for x in (lengths, latent, up_key, queries)])


def in_hbm(x):
    return pltpu.with_memory_space_constraint(x, pltpu.HBM)


def slot_kernel(dests, lat, after, outgoing, table, sem):
    count, block_len, width = lat.shape
    rank = width // 2
    first = pl.multiple_of(lax.axis_index(SEQ) * count, count)
    copy = pltpu.make_async_copy(dests.at[pl.ds(first, count)], table, sem)
    copy.start()
    copy.wait()
    for b in range(count):
        to = (table[b] & 1) * (count // 2) + (table[b] >> 1)
        outgoing[to, :block_len, :] = lat[b, :, :rank]
        outgoing[to, block_len : 2 * block_len, :] = lat[b, :, rank:]


def slot(block_dest, lat, after, extra):
    count, block_len, width = lat.shape
    return pl.pallas_call(
        slot_kernel,
        out_shape=jax.ShapeDtypeStruct((count, 2 * block_len + extra, width // 2), lat.dtype),
        in_specs=[HBM, VMEM, VMEM],
        out_specs=VMEM,
        scratch_shapes=[pltpu.SMEM((count,), jnp.int32), pltpu.SemaphoreType.DMA],
        compiler_params=PARAMS,
        name="slot",
    )(in_hbm(block_dest), lat, after)


def joined(first, second):
    largest = jnp.maximum(first[1], second[1])
    factor_a = jnp.exp(first[1] - largest)
    factor_b = jnp.exp(second[1] - largest)
    accum = first[0] * factor_a + second[0] * factor_b
    return (accum, largest, first[2] * factor_a + second[2] * factor_b)


def half_kept():
    return (lax.axis_index("seq_2") + lax.axis_index("seq_1")) % 2


def merge_kernel(mine, theirs, out):
    kept = out.shape[1]
    rows = pl.ds(pl.multiple_of(half_kept() * kept, kept), kept)
    both = joined(
        [mine[i, rows, :] for i in range(3)], [theirs[i, rows, :] for i in range(3)]
    )
    for i in range(3):
        out[i] = both[i]


def merge(mine, theirs):
    return pl.pallas_call(
        merge_kernel,
        out_shape=jax.ShapeDtypeStruct((3, mine.shape[1] // 2, mine.shape[2]), jnp.float32),
        in_specs=[VMEM, VMEM],
        out_specs=VMEM,
        compiler_params=PARAMS,
        name="merge",
    )(mine, theirs)


def pack_kernel(mine, theirs, up_value, _, out):
    head_dim = mine.shape[2]
    accum, _, total = joined([mine[i] for i in range(3)], [theirs[i] for i in range(3)])
    mean = accum / total
    half = mean.shape[0] // 2
    mean = jnp.where(lax.axis_index("seq_1") % 2 == 1, mean[half:], mean[:half])
    value_map = up_value[lax.axis_index("grp")]
    value_map = jnp.where(
        half_kept() == 1, value_map[:, head_dim:], value_map[:, :head_dim]
    )
    wide = lax.dot_general(
        split(mean, 3), value_map, (((1,), (0,)), ((), ())), preferred_element_type=jnp.float32
    )
    extra = split(wide[2 * half :] + wide[half : 2 * half] + wide[:half], 2)
    rows = out.shape[1] - extra.shape[0]
    for b in range(out.shape[0]):
        out[b, rows:, :] = extra


def pack(mine, theirs, up_value, outgoing):
    return pl.pallas_call(
        pack_kernel,
        out_shape=jax.ShapeDtypeStruct(outgoing.shape, outgoing.dtype),
        in_specs=[VMEM] * 4,
        out_specs=VMEM,
        input_output_aliases={3: 0},
        compiler_params=PARAMS,
        name="pack",
    )(mine, theirs, up_value, outgoing)


def unpack_kernel(received, decode, attended, rows_out, sems, row_sems):
    sources, rows, rank = received.shape
    _, groups, chips, cores, block_len, _ = decode.shape
    copies = []
    for g in range(groups):
        for c in range(cores):
            for k in range(2):
                sent = pl.ds((c * groups + g) * chips, chips)
                copies.append(
                    pltpu.make_async_copy(
                        received.at[sent, pl.ds(k * block_len, block_len), :],
                        decode.at[0, g, :, c, :, pl.ds(k * rank, rank)],
                        sems.at[g, c, k],
                    )
                )
    for c in copies:
        c.start()
    half = (rows - 2 * block_len) // 2
    span = rows_out.shape[1] // groups
    for g in range(groups):
        for s in range(chips * cores):
            chip, c = s // cores, s % cores
            x, y = chip // 4, chip % 4
            seq = 2 * x + y // 2
            part = received[(c * groups + g) * chips + chip, 2 * block_len :, :]
            part = part.astype(jnp.float32)
            part = part[half:] + part[:half]
            first = g * 16 + (c + y) % 2 * 8 + y % 2 * 4
            for j in range(half):
                at = (first + j) * rank
                rows_out[seq : seq + 1, at : at + rank] = part[j : j + 1]
        columns = pl.ds(g * span, span)
        copy = pltpu.make_async_copy(
            rows_out.at[:, columns], attended.at[:, columns], row_sems.at[g]
        )
        copy.start()
        copies.append(copy)
    for c in copies:
        c.wait()


def unpack(received, groups, batch, heads, block_len):
    sources, _, rank = received.shape
    return pl.pallas_call(
        unpack_kernel,
        out_shape=(
            jax.ShapeDtypeStruct(
                (1, groups, sources // groups // 2, 2, block_len, 2 * rank), received.dtype
            ),
            jax.ShapeDtypeStruct((batch, heads * rank), jnp.float32),
        ),
        in_specs=[VMEM],
        out_specs=(HBM, HBM),
        scratch_shapes=[
            pltpu.VMEM((batch, heads * rank), jnp.float32),
            pltpu.SemaphoreType.DMA((groups, 2, 2)),
            pltpu.SemaphoreType.DMA((groups,)),
        ],
        compiler_params=PARAMS,
        name="unpack",
    )(received)


def swap(x, axes, mask):
    return lax.ppermute(x, axes, [(i, i ^ mask) for i in range(lax.axis_size(axes))])


def body(latent, up_key, up_value, queries, lengths, block_dest):
    groups = up_key.shape[0]
    block_len = latent.shape[2]
    batch, q_heads, _ = queries.shape
    part, lat = attend(latent[0], up_key, queries, lengths, 2)
    part = merge(part, swap(part, "seq_2", 1))
    outgoing = slot(block_dest, lat, part, 8)
    outgoing = pack(part, swap(part, ("seq_1", "seq_2"), 3), up_value, outgoing)
    received = lax.all_to_all(outgoing, EXCHANGE, split_axis=0, concat_axis=0, tiled=True)
    decode, attended = unpack(received, groups, batch, q_heads, block_len)
    return (decode.reshape(1, groups, -1, *latent.shape[2:]), attended)


def solution(mesh):
    finer = Mesh(
        mesh.devices.reshape(mesh.shape["grp"], 4, 4, 2), ("grp", "seq_0", "seq_1", "seq_2")
    )
    in_specs = (P("grp", SEQ, None, None), P(), P(), P(), P(), P())
    out_specs = (P(GRP_SEQ, None, None, None, None), P())
    return jax.shard_map(body, mesh=finer, in_specs=in_specs, out_specs=out_specs, check_vma=False)
```

```python
import jax
import jax.numpy as jnp
from jax import lax
from jax.experimental import pallas as pl
from jax.experimental.pallas import tpu as pltpu
from jax.sharding import Mesh
from jax.sharding import PartitionSpec as P

SEQ = ("seq_0", "seq_1", "seq_2")
GRP_SEQ = ("grp", "seq_0", "seq_1", "seq_2")
EXCHANGE = ("seq_2", "grp", "seq_0", "seq_1")
NEG = -1e30
VMEM = pl.BlockSpec(memory_space=pltpu.VMEM)
HBM = pl.BlockSpec(memory_space=pltpu.HBM)
PARAMS = pltpu.CompilerParams(vmem_limit_bytes=16 << 20)


def split(x, parts):
    pieces = []
    for _ in range(parts):
        piece = x.astype(jnp.bfloat16).astype(jnp.float32)
        pieces.append(piece)
        x = x - piece
    return jnp.concatenate(pieces, axis=0).astype(jnp.bfloat16)


def attend_kernel(ends, latent, up_key, queries, out, lat, key_map, query, lengths, sems):
    count, block_len, width = lat.shape
    chunks = sems.shape[0] - 3
    blocks = count // chunks
    tokens = blocks * block_len
    rank = width // 2
    heads, head_dim = query.shape
    per_group = key_map.shape[1] // head_dim
    per_kv = heads // per_group
    shard = lax.axis_index(SEQ)
    group = lax.axis_index("grp")
    quarter = lax.axis_size(SEQ) // queries.shape[0]
    seq = shard // quarter
    first = pl.multiple_of(group * heads, heads)
    small = [
        pltpu.make_async_copy(queries.at[seq, pl.ds(first, heads)], query, sems.at[0]),
        pltpu.make_async_copy(up_key.at[group], key_map, sems.at[1]),
        pltpu.make_async_copy(ends, lengths, sems.at[2]),
    ]
    parts = [pl.ds(i * blocks, blocks) for i in range(chunks)]
    large = [
        pltpu.make_async_copy(latent.at[part], lat.at[part], sems.at[3 + i])
        for i, part in enumerate(parts)
    ]
    for copy in small + large:
        copy.start()
    for copy in small:
        copy.wait()
    live_count = lengths[seq] - (shard % quarter) * (count * block_len)
    heads_f = query[...].astype(jnp.float32)
    rows = [
        lax.dot_general(
            heads_f[k * per_kv : (k + 1) * per_kv].astype(jnp.bfloat16),
            key_map[:, k * head_dim : (k + 1) * head_dim],
            (((1,), (1,)), ((), ())),
            preferred_element_type=jnp.float32,
        )
        for k in range(per_group)
    ]
    absorbed = split(jnp.concatenate(rows, axis=0) * (1.0 / float(head_dim) ** 0.5), 3)

    def scored(i):
        raw = lax.dot_general(
            absorbed,
            lat[parts[i], :, :rank].reshape(tokens, rank),
            (((1,), (1,)), ((), ())),
            preferred_element_type=jnp.float32,
        )
        scores = raw[2 * heads :] + raw[heads : 2 * heads] + raw[:heads]
        position = lax.broadcasted_iota(jnp.int32, (heads, tokens), 1) + i * tokens
        live = position < live_count
        return (jnp.where(live, scores, NEG), live)

    def weighed(scores, live):
        largest = jnp.max(scores, axis=1, keepdims=True)
        weights = jnp.where(live, jnp.exp(scores - largest), 0.0)
        return (split(weights, 2), largest, jnp.sum(weights, axis=1, keepdims=True))

    def summed(i, halves, largest, total):
        both = lax.dot_general(
            halves,
            lat[parts[i], :, rank:].reshape(tokens, rank),
            (((1,), (0,)), ((), ())),
            preferred_element_type=jnp.float32,
        )
        return (both[:heads] + both[heads:], largest, total)

    scores, weights, found = ({}, {}, [])
    for step in range(chunks + 2):
        if step < chunks:
            large[step].wait()
            scores[step] = scored(step)
        if 0 <= step - 1 < chunks:
            weights[step - 1] = weighed(*scores.pop(step - 1))
        if step >= 2:
            found.append(summed(step - 2, *weights.pop(step - 2)))
    largest = found[0][1]
    for chunk in found[1:]:
        largest = jnp.maximum(largest, chunk[1])
    factors = [jnp.exp(f[1] - largest) for f in found]
    out[0] = sum(f[0] * k for f, k in zip(found, factors))
    out[1] = jnp.broadcast_to(largest, (heads, rank))
    out[2] = jnp.broadcast_to(sum(f[2] * k for f, k in zip(found, factors)), (heads, rank))


def attend(latent, up_key, queries, lengths, chunks):
    heads = queries.shape[1] // up_key.shape[0]
    return pl.pallas_call(
        attend_kernel,
        out_shape=(
            jax.ShapeDtypeStruct((3, heads, latent.shape[2] // 2), jnp.float32),
            jax.ShapeDtypeStruct(latent.shape, latent.dtype),
        ),
        in_specs=[HBM] * 4,
        out_specs=(VMEM,) * 2,
        scratch_shapes=[
            pltpu.VMEM(up_key.shape[1:], up_key.dtype),
            pltpu.VMEM((heads, queries.shape[2]), queries.dtype),
            pltpu.SMEM(lengths.shape, jnp.int32),
            pltpu.SemaphoreType.DMA((3 + chunks,)),
        ],
        compiler_params=PARAMS,
        name="attend",
    )(*[in_hbm(x) for x in (lengths, latent, up_key, queries)])


def in_hbm(x):
    return pltpu.with_memory_space_constraint(x, pltpu.HBM)


def slot_kernel(dests, lat, after, outgoing, table, sem):
    count, block_len, width = lat.shape
    rank = width // 2
    first = pl.multiple_of(lax.axis_index(SEQ) * count, count)
    copy = pltpu.make_async_copy(dests.at[pl.ds(first, count)], table, sem)
    copy.start()
    copy.wait()
    for b in range(count):
        to = (table[b] & 1) * (count // 2) + (table[b] >> 1)
        outgoing[to, :block_len, :] = lat[b, :, :rank]
        outgoing[to, block_len : 2 * block_len, :] = lat[b, :, rank:]


def slot(block_dest, lat, after, extra):
    count, block_len, width = lat.shape
    return pl.pallas_call(
        slot_kernel,
        out_shape=jax.ShapeDtypeStruct((count, 2 * block_len + extra, width // 2), lat.dtype),
        in_specs=[HBM, VMEM, VMEM],
        out_specs=VMEM,
        scratch_shapes=[pltpu.SMEM((count,), jnp.int32), pltpu.SemaphoreType.DMA],
        compiler_params=PARAMS,
        name="slot",
    )(in_hbm(block_dest), lat, after)


def joined(first, second):
    largest = jnp.maximum(first[1], second[1])
    factor_a = jnp.exp(first[1] - largest)
    factor_b = jnp.exp(second[1] - largest)
    accum = first[0] * factor_a + second[0] * factor_b
    return (accum, largest, first[2] * factor_a + second[2] * factor_b)


def half_kept():
    return (lax.axis_index("seq_2") + lax.axis_index("seq_1")) % 2


def merge_kernel(mine, theirs, out):
    kept = out.shape[1]
    rows = pl.ds(pl.multiple_of(half_kept() * kept, kept), kept)
    both = joined(
        [mine[i, rows, :] for i in range(3)], [theirs[i, rows, :] for i in range(3)]
    )
    for i in range(3):
        out[i] = both[i]


def merge(mine, theirs):
    return pl.pallas_call(
        merge_kernel,
        out_shape=jax.ShapeDtypeStruct((3, mine.shape[1] // 2, mine.shape[2]), jnp.float32),
        in_specs=[VMEM, VMEM],
        out_specs=VMEM,
        compiler_params=PARAMS,
        name="merge",
    )(mine, theirs)


def pack_kernel(mine, theirs, up_value, _, out):
    head_dim = mine.shape[2]
    accum, _, total = joined([mine[i] for i in range(3)], [theirs[i] for i in range(3)])
    mean = accum / total
    half = mean.shape[0] // 2
    mean = jnp.where(lax.axis_index("seq_1") % 2 == 1, mean[half:], mean[:half])
    value_map = up_value[lax.axis_index("grp")]
    value_map = jnp.where(
        half_kept() == 1, value_map[:, head_dim:], value_map[:, :head_dim]
    )
    wide = lax.dot_general(
        split(mean, 3), value_map, (((1,), (0,)), ((), ())), preferred_element_type=jnp.float32
    )
    extra = split(wide[2 * half :] + wide[half : 2 * half] + wide[:half], 2)
    rows = out.shape[1] - extra.shape[0]
    for b in range(out.shape[0]):
        out[b, rows:, :] = extra


def pack(mine, theirs, up_value, outgoing):
    return pl.pallas_call(
        pack_kernel,
        out_shape=jax.ShapeDtypeStruct(outgoing.shape, outgoing.dtype),
        in_specs=[VMEM] * 4,
        out_specs=VMEM,
        input_output_aliases={3: 0},
        compiler_params=PARAMS,
        name="pack",
    )(mine, theirs, up_value, pltpu.with_memory_space_constraint(outgoing, pltpu.VMEM))


def unpack_kernel(received, decode, attended, rows_out, sems, row_sems):
    sources, rows, rank = received.shape
    _, groups, chips, cores, block_len, _ = decode.shape
    copies = []
    for g in range(groups):
        for c in range(cores):
            for k in range(2):
                sent = pl.ds((c * groups + g) * chips, chips)
                copies.append(
                    pltpu.make_async_copy(
                        received.at[sent, pl.ds(k * block_len, block_len), :],
                        decode.at[0, g, :, c, :, pl.ds(k * rank, rank)],
                        sems.at[g, c, k],
                    )
                )
    for c in copies:
        c.start()
    half = (rows - 2 * block_len) // 2
    span = rows_out.shape[1] // groups
    for g in range(groups):
        for s in range(chips * cores):
            chip, c = s // cores, s % cores
            x, y = chip // 4, chip % 4
            seq = 2 * x + y // 2
            part = received[(c * groups + g) * chips + chip, 2 * block_len :, :]
            part = part.astype(jnp.float32)
            part = part[half:] + part[:half]
            first = g * 16 + (c + y) % 2 * 8 + y % 2 * 4
            for j in range(half):
                at = (first + j) * rank
                rows_out[seq : seq + 1, at : at + rank] = part[j : j + 1]
        columns = pl.ds(g * span, span)
        copy = pltpu.make_async_copy(
            rows_out.at[:, columns], attended.at[:, columns], row_sems.at[g]
        )
        copy.start()
        copies.append(copy)
    for c in copies:
        c.wait()


def unpack(received, groups, batch, heads, block_len):
    sources, _, rank = received.shape
    return pl.pallas_call(
        unpack_kernel,
        out_shape=(
            jax.ShapeDtypeStruct(
                (1, groups, sources // groups // 2, 2, block_len, 2 * rank), received.dtype
            ),
            jax.ShapeDtypeStruct((batch, heads * rank), jnp.float32),
        ),
        in_specs=[VMEM],
        out_specs=(HBM, HBM),
        scratch_shapes=[
            pltpu.VMEM((batch, heads * rank), jnp.float32),
            pltpu.SemaphoreType.DMA((groups, 2, 2)),
            pltpu.SemaphoreType.DMA((groups,)),
        ],
        compiler_params=PARAMS,
        name="unpack",
    )(received)


def swap(x, axes, mask):
    return lax.ppermute(x, axes, [(i, i ^ mask) for i in range(lax.axis_size(axes))])


def body(latent, up_key, up_value, queries, lengths, block_dest):
    groups = up_key.shape[0]
    block_len = latent.shape[2]
    batch, q_heads, _ = queries.shape
    part, lat = attend(latent[0], up_key, queries, lengths, 2)
    part = merge(part, swap(part, "seq_2", 1))
    outgoing = slot(block_dest, lat, part, 8)
    outgoing = pack(part, swap(part, ("seq_1", "seq_2"), 3), up_value, outgoing)
    received = lax.all_to_all(outgoing, EXCHANGE, split_axis=0, concat_axis=0, tiled=True)
    decode, attended = unpack(received, groups, batch, q_heads, block_len)
    return (decode.reshape(1, groups, -1, *latent.shape[2:]), attended)


def solution(mesh):
    finer = Mesh(
        mesh.devices.reshape(mesh.shape["grp"], 4, 4, 2), ("grp", "seq_0", "seq_1", "seq_2")
    )
    in_specs = (P("grp", SEQ, None, None), P(), P(), P(), P(), P())
    out_specs = (P(GRP_SEQ, None, None, None, None), P())
    return jax.shard_map(body, mesh=finer, in_specs=in_specs, out_specs=out_specs, check_vma=False)
```

```python
import jax
import jax.numpy as jnp
from jax import lax
from jax.experimental import pallas as pl
from jax.experimental.pallas import tpu as pltpu
from jax.sharding import Mesh
from jax.sharding import PartitionSpec as P

SEQ = ("seq_0", "seq_1", "seq_2")
GRP_SEQ = ("grp", "seq_0", "seq_1", "seq_2")
EXCHANGE = ("seq_2", "grp", "seq_1", "seq_0")
NEG = -1e30
VMEM = pl.BlockSpec(memory_space=pltpu.VMEM)
HBM = pl.BlockSpec(memory_space=pltpu.HBM)
PARAMS = pltpu.CompilerParams(vmem_limit_bytes=16 << 20)


def split(x, parts):
    pieces = []
    for _ in range(parts):
        piece = x.astype(jnp.bfloat16).astype(jnp.float32)
        pieces.append(piece)
        x = x - piece
    return jnp.concatenate(pieces, axis=0).astype(jnp.bfloat16)


def attend_kernel(ends, latent, up_key, queries, out, lat, key_map, query, lengths, sems):
    count, block_len, width = lat.shape
    chunks = sems.shape[0] - 3
    blocks = count // chunks
    tokens = blocks * block_len
    rank = width // 2
    heads, head_dim = query.shape
    per_group = key_map.shape[1] // head_dim
    per_kv = heads // per_group
    shard = lax.axis_index(SEQ)
    group = lax.axis_index("grp")
    quarter = lax.axis_size(SEQ) // queries.shape[0]
    seq = shard // quarter
    first = pl.multiple_of(group * heads, heads)
    small = [
        pltpu.make_async_copy(queries.at[seq, pl.ds(first, heads)], query, sems.at[0]),
        pltpu.make_async_copy(up_key.at[group], key_map, sems.at[1]),
        pltpu.make_async_copy(ends, lengths, sems.at[2]),
    ]
    parts = [pl.ds(i * blocks, blocks) for i in range(chunks)]
    large = [
        pltpu.make_async_copy(latent.at[part], lat.at[part], sems.at[3 + i])
        for i, part in enumerate(parts)
    ]
    for copy in small + large:
        copy.start()
    for copy in small:
        copy.wait()
    live_count = lengths[seq] - (shard % quarter) * (count * block_len)
    heads_f = query[...].astype(jnp.float32)
    rows = [
        lax.dot_general(
            heads_f[k * per_kv : (k + 1) * per_kv].astype(jnp.bfloat16),
            key_map[:, k * head_dim : (k + 1) * head_dim],
            (((1,), (1,)), ((), ())),
            preferred_element_type=jnp.float32,
        )
        for k in range(per_group)
    ]
    absorbed = split(jnp.concatenate(rows, axis=0) * (1.0 / float(head_dim) ** 0.5), 3)

    def scored(i):
        raw = lax.dot_general(
            absorbed,
            lat[parts[i], :, :rank].reshape(tokens, rank),
            (((1,), (1,)), ((), ())),
            preferred_element_type=jnp.float32,
        )
        scores = raw[2 * heads :] + raw[heads : 2 * heads] + raw[:heads]
        position = lax.broadcasted_iota(jnp.int32, (heads, tokens), 1) + i * tokens
        live = position < live_count
        return (jnp.where(live, scores, NEG), live)

    def weighed(scores, live):
        largest = jnp.max(scores, axis=1, keepdims=True)
        weights = jnp.where(live, jnp.exp(scores - largest), 0.0)
        return (split(weights, 2), largest, jnp.sum(weights, axis=1, keepdims=True))

    def summed(i, halves, largest, total):
        both = lax.dot_general(
            halves,
            lat[parts[i], :, rank:].reshape(tokens, rank),
            (((1,), (0,)), ((), ())),
            preferred_element_type=jnp.float32,
        )
        return (both[:heads] + both[heads:], largest, total)

    scores, weights, found = ({}, {}, [])
    for step in range(chunks + 2):
        if step < chunks:
            large[step].wait()
            scores[step] = scored(step)
        if 0 <= step - 1 < chunks:
            weights[step - 1] = weighed(*scores.pop(step - 1))
        if step >= 2:
            found.append(summed(step - 2, *weights.pop(step - 2)))
    largest = found[0][1]
    for chunk in found[1:]:
        largest = jnp.maximum(largest, chunk[1])
    factors = [jnp.exp(f[1] - largest) for f in found]
    out[0] = sum(f[0] * k for f, k in zip(found, factors))
    out[1] = jnp.broadcast_to(largest, (heads, rank))
    out[2] = jnp.broadcast_to(sum(f[2] * k for f, k in zip(found, factors)), (heads, rank))


def attend(latent, up_key, queries, lengths, chunks):
    heads = queries.shape[1] // up_key.shape[0]
    return pl.pallas_call(
        attend_kernel,
        out_shape=(
            jax.ShapeDtypeStruct((3, heads, latent.shape[2] // 2), jnp.float32),
            jax.ShapeDtypeStruct(latent.shape, latent.dtype),
        ),
        in_specs=[HBM] * 4,
        out_specs=(VMEM,) * 2,
        scratch_shapes=[
            pltpu.VMEM(up_key.shape[1:], up_key.dtype),
            pltpu.VMEM((heads, queries.shape[2]), queries.dtype),
            pltpu.SMEM(lengths.shape, jnp.int32),
            pltpu.SemaphoreType.DMA((3 + chunks,)),
        ],
        compiler_params=PARAMS,
        name="attend",
    )(*[in_hbm(x) for x in (lengths, latent, up_key, queries)])


def in_hbm(x):
    return pltpu.with_memory_space_constraint(x, pltpu.HBM)


def slot_kernel(dests, lat, after, outgoing, table, sem):
    count, block_len, width = lat.shape
    rank = width // 2
    first = pl.multiple_of(lax.axis_index(SEQ) * count, count)
    copy = pltpu.make_async_copy(dests.at[pl.ds(first, count)], table, sem)
    copy.start()
    copy.wait()
    for b in range(count):
        d = table[b]
        to = (d & 1) * 64 + (d >> 5) * 16 + ((d >> 1) & 3) * 4 + ((d >> 3) & 3)
        outgoing[to, :block_len, :] = lat[b, :, :rank]
        outgoing[to, block_len : 2 * block_len, :] = lat[b, :, rank:]


def slot(block_dest, lat, after, extra):
    count, block_len, width = lat.shape
    return pl.pallas_call(
        slot_kernel,
        out_shape=jax.ShapeDtypeStruct((count, 2 * block_len + extra, width // 2), lat.dtype),
        in_specs=[HBM, VMEM, VMEM],
        out_specs=VMEM,
        scratch_shapes=[pltpu.SMEM((count,), jnp.int32), pltpu.SemaphoreType.DMA],
        compiler_params=PARAMS,
        name="slot",
    )(in_hbm(block_dest), lat, after)


def joined(first, second):
    largest = jnp.maximum(first[1], second[1])
    factor_a = jnp.exp(first[1] - largest)
    factor_b = jnp.exp(second[1] - largest)
    accum = first[0] * factor_a + second[0] * factor_b
    return (accum, largest, first[2] * factor_a + second[2] * factor_b)


def half_kept():
    return (lax.axis_index("seq_2") + lax.axis_index("seq_1")) % 2


def merge_kernel(mine, theirs, out):
    kept = out.shape[1]
    rows = pl.ds(pl.multiple_of(half_kept() * kept, kept), kept)
    both = joined(
        [mine[i, rows, :] for i in range(3)], [theirs[i, rows, :] for i in range(3)]
    )
    for i in range(3):
        out[i] = both[i]


def merge(mine, theirs):
    return pl.pallas_call(
        merge_kernel,
        out_shape=jax.ShapeDtypeStruct((3, mine.shape[1] // 2, mine.shape[2]), jnp.float32),
        in_specs=[VMEM, VMEM],
        out_specs=VMEM,
        compiler_params=PARAMS,
        name="merge",
    )(mine, theirs)


def pack_kernel(mine, theirs, up_value, _, out):
    head_dim = mine.shape[2]
    accum, _, total = joined([mine[i] for i in range(3)], [theirs[i] for i in range(3)])
    mean = accum / total
    half = mean.shape[0] // 2
    mean = jnp.where(lax.axis_index("seq_1") % 2 == 1, mean[half:], mean[:half])
    value_map = up_value[lax.axis_index("grp")]
    value_map = jnp.where(
        half_kept() == 1, value_map[:, head_dim:], value_map[:, :head_dim]
    )
    wide = lax.dot_general(
        split(mean, 3), value_map, (((1,), (0,)), ((), ())), preferred_element_type=jnp.float32
    )
    extra = split(wide[2 * half :] + wide[half : 2 * half] + wide[:half], 2)
    rows = out.shape[1] - extra.shape[0]
    for b in range(out.shape[0]):
        out[b, rows:, :] = extra


def pack(mine, theirs, up_value, outgoing):
    return pl.pallas_call(
        pack_kernel,
        out_shape=jax.ShapeDtypeStruct(outgoing.shape, outgoing.dtype),
        in_specs=[VMEM] * 4,
        out_specs=VMEM,
        input_output_aliases={3: 0},
        compiler_params=PARAMS,
        name="pack",
    )(mine, theirs, up_value, pltpu.with_memory_space_constraint(outgoing, pltpu.VMEM))


def unpack_kernel(received, decode, attended, rows_out, sems, row_sems):
    cores, groups, high, wide, rows, rank = received.shape
    block_len = decode.shape[5]
    copies = []
    for c in range(cores):
        for y in range(high):
            for k in range(2):
                copies.append(
                    pltpu.make_async_copy(
                        received.at[c, :, y, :, pl.ds(k * block_len, block_len), :],
                        decode.at[0, :, :, y, c, :, pl.ds(k * rank, rank)],
                        sems.at[c, y, k],
                    )
                )
    for c in copies:
        c.start()
    half = (rows - 2 * block_len) // 2
    span = rows_out.shape[1] // groups
    for g in range(groups):
        for s in range(wide * high * cores):
            x, y, c = s // (high * cores), s // cores % high, s % cores
            seq = 2 * x + y // 2
            part = received[c, g, y, x, 2 * block_len :, :]
            part = part.astype(jnp.float32)
            part = part[half:] + part[:half]
            first = g * 16 + (c + y) % 2 * 8 + y % 2 * 4
            for j in range(half):
                at = (first + j) * rank
                rows_out[seq : seq + 1, at : at + rank] = part[j : j + 1]
        columns = pl.ds(g * span, span)
        copy = pltpu.make_async_copy(
            rows_out.at[:, columns], attended.at[:, columns], row_sems.at[g]
        )
        copy.start()
        copies.append(copy)
    for c in copies:
        c.wait()


def unpack(received, groups, batch, heads, block_len):
    _, rows, rank = received.shape
    received = received.reshape(2, groups, 4, 4, rows, rank)
    return pl.pallas_call(
        unpack_kernel,
        out_shape=(
            jax.ShapeDtypeStruct(
                (1, groups, 4, 4, 2, block_len, 2 * rank), received.dtype
            ),
            jax.ShapeDtypeStruct((batch, heads * rank), jnp.float32),
        ),
        in_specs=[VMEM],
        out_specs=(HBM, HBM),
        scratch_shapes=[
            pltpu.VMEM((batch, heads * rank), jnp.float32),
            pltpu.SemaphoreType.DMA((2, 4, 2)),
            pltpu.SemaphoreType.DMA((groups,)),
        ],
        compiler_params=PARAMS,
        name="unpack",
    )(received)


def swap(x, axes, mask):
    return lax.ppermute(x, axes, [(i, i ^ mask) for i in range(lax.axis_size(axes))])


def body(latent, up_key, up_value, queries, lengths, block_dest):
    groups = up_key.shape[0]
    block_len = latent.shape[2]
    batch, q_heads, _ = queries.shape
    part, lat = attend(latent[0], up_key, queries, lengths, 2)
    part = merge(part, swap(part, "seq_2", 1))
    outgoing = slot(block_dest, lat, part, 8)
    outgoing = pack(part, swap(part, ("seq_1", "seq_2"), 3), up_value, outgoing)
    received = lax.all_to_all(outgoing, EXCHANGE, split_axis=0, concat_axis=0, tiled=True)
    decode, attended = unpack(received, groups, batch, q_heads, block_len)
    return (decode.reshape(1, groups, -1, *latent.shape[2:]), attended)


def solution(mesh):
    finer = Mesh(
        mesh.devices.reshape(mesh.shape["grp"], 4, 4, 2), ("grp", "seq_0", "seq_1", "seq_2")
    )
    in_specs = (P("grp", SEQ, None, None), P(), P(), P(), P(), P())
    out_specs = (P(GRP_SEQ, None, None, None, None), P())
    return jax.shard_map(body, mesh=finer, in_specs=in_specs, out_specs=out_specs, check_vma=False)
```

```python
import jax
import jax.numpy as jnp
from jax import lax
from jax.experimental import pallas as pl
from jax.experimental.pallas import tpu as pltpu
from jax.sharding import Mesh
from jax.sharding import PartitionSpec as P

SEQ = ("seq_0", "seq_1", "seq_2")
GRP_SEQ = ("grp", "seq_0", "seq_1", "seq_2")
EXCHANGE = ("seq_2", "grp", "seq_1", "seq_0")
NEG = -1e30
VMEM = pl.BlockSpec(memory_space=pltpu.VMEM)
HBM = pl.BlockSpec(memory_space=pltpu.HBM)
PARAMS = pltpu.CompilerParams(vmem_limit_bytes=16 << 20)


def split(x, parts):
    pieces = []
    for _ in range(parts):
        piece = x.astype(jnp.bfloat16).astype(jnp.float32)
        pieces.append(piece)
        x = x - piece
    return jnp.concatenate(pieces, axis=0).astype(jnp.bfloat16)


def attend_kernel(ends, latent, up_key, queries, out, lat, key_map, query, lengths, sems):
    count, block_len, width = lat.shape
    chunks = sems.shape[0] - 3
    blocks = count // chunks
    tokens = blocks * block_len
    rank = width // 2
    heads, head_dim = query.shape
    per_group = key_map.shape[1] // head_dim
    per_kv = heads // per_group
    shard = lax.axis_index(SEQ)
    group = lax.axis_index("grp")
    quarter = lax.axis_size(SEQ) // queries.shape[0]
    seq = shard // quarter
    first = pl.multiple_of(group * heads, heads)
    small = [
        pltpu.make_async_copy(queries.at[seq, pl.ds(first, heads)], query, sems.at[0]),
        pltpu.make_async_copy(up_key.at[group], key_map, sems.at[1]),
        pltpu.make_async_copy(ends, lengths, sems.at[2]),
    ]
    parts = [pl.ds(i * blocks, blocks) for i in range(chunks)]
    large = [
        pltpu.make_async_copy(latent.at[part], lat.at[part], sems.at[3 + i])
        for i, part in enumerate(parts)
    ]
    for copy in small + large:
        copy.start()
    for copy in small:
        copy.wait()
    live_count = lengths[seq] - (shard % quarter) * (count * block_len)
    heads_f = query[...].astype(jnp.float32)
    rows = [
        lax.dot_general(
            heads_f[k * per_kv : (k + 1) * per_kv].astype(jnp.bfloat16),
            key_map[:, k * head_dim : (k + 1) * head_dim],
            (((1,), (1,)), ((), ())),
            preferred_element_type=jnp.float32,
        )
        for k in range(per_group)
    ]
    absorbed = split(jnp.concatenate(rows, axis=0) * (1.0 / float(head_dim) ** 0.5), 3)

    def scored(i):
        raw = lax.dot_general(
            absorbed,
            lat[parts[i], :, :rank].reshape(tokens, rank),
            (((1,), (1,)), ((), ())),
            preferred_element_type=jnp.float32,
        )
        scores = raw[2 * heads :] + raw[heads : 2 * heads] + raw[:heads]
        position = lax.broadcasted_iota(jnp.int32, (heads, tokens), 1) + i * tokens
        live = position < live_count
        return (jnp.where(live, scores, NEG), live)

    def weighed(scores, live):
        largest = jnp.max(scores, axis=1, keepdims=True)
        weights = jnp.where(live, jnp.exp(scores - largest), 0.0)
        return (split(weights, 2), largest, jnp.sum(weights, axis=1, keepdims=True))

    def summed(i, halves, largest, total):
        both = lax.dot_general(
            halves,
            lat[parts[i], :, rank:].reshape(tokens, rank),
            (((1,), (0,)), ((), ())),
            preferred_element_type=jnp.float32,
        )
        return (both[:heads] + both[heads:], largest, total)

    scores, weights, found = ({}, {}, [])
    for step in range(chunks + 2):
        if step < chunks:
            large[step].wait()
            scores[step] = scored(step)
        if 0 <= step - 1 < chunks:
            weights[step - 1] = weighed(*scores.pop(step - 1))
        if step >= 2:
            found.append(summed(step - 2, *weights.pop(step - 2)))
    largest = found[0][1]
    for chunk in found[1:]:
        largest = jnp.maximum(largest, chunk[1])
    factors = [jnp.exp(f[1] - largest) for f in found]
    out[0] = sum(f[0] * k for f, k in zip(found, factors))
    out[1] = jnp.broadcast_to(largest, (heads, rank))
    out[2] = jnp.broadcast_to(sum(f[2] * k for f, k in zip(found, factors)), (heads, rank))


def attend(latent, up_key, queries, lengths, chunks):
    heads = queries.shape[1] // up_key.shape[0]
    return pl.pallas_call(
        attend_kernel,
        out_shape=(
            jax.ShapeDtypeStruct((3, heads, latent.shape[2] // 2), jnp.float32),
            jax.ShapeDtypeStruct(latent.shape, latent.dtype),
        ),
        in_specs=[HBM] * 4,
        out_specs=(VMEM,) * 2,
        scratch_shapes=[
            pltpu.VMEM(up_key.shape[1:], up_key.dtype),
            pltpu.VMEM((heads, queries.shape[2]), queries.dtype),
            pltpu.SMEM(lengths.shape, jnp.int32),
            pltpu.SemaphoreType.DMA((3 + chunks,)),
        ],
        compiler_params=PARAMS,
        name="attend",
    )(*[in_hbm(x) for x in (lengths, latent, up_key, queries)])


def in_hbm(x):
    return pltpu.with_memory_space_constraint(x, pltpu.HBM)


def slot_kernel(dests, lat, after, outgoing, table, sem):
    count, block_len, width = lat.shape
    rank = width // 2
    first = pl.multiple_of(lax.axis_index(SEQ) * count, count)
    copy = pltpu.make_async_copy(dests.at[pl.ds(first, count)], table, sem)
    copy.start()
    copy.wait()
    for b in range(count):
        d = table[b]
        to = (d & 1) * 64 + (d >> 5) * 16 + ((d >> 1) & 3) * 4 + ((d >> 3) & 3)
        outgoing[to, :block_len, :] = lat[b, :, :rank]
        outgoing[to, block_len : 2 * block_len, :] = lat[b, :, rank:]


def slot(block_dest, lat, after, extra):
    count, block_len, width = lat.shape
    return pl.pallas_call(
        slot_kernel,
        out_shape=jax.ShapeDtypeStruct((count, 2 * block_len + extra, width // 2), lat.dtype),
        in_specs=[HBM, VMEM, VMEM],
        out_specs=VMEM,
        scratch_shapes=[pltpu.SMEM((count,), jnp.int32), pltpu.SemaphoreType.DMA],
        compiler_params=PARAMS,
        name="slot",
    )(in_hbm(block_dest), lat, after)


def joined(first, second):
    largest = jnp.maximum(first[1], second[1])
    factor_a = jnp.exp(first[1] - largest)
    factor_b = jnp.exp(second[1] - largest)
    accum = first[0] * factor_a + second[0] * factor_b
    return (accum, largest, first[2] * factor_a + second[2] * factor_b)


def half_kept():
    return (lax.axis_index("seq_2") + lax.axis_index("seq_1")) % 2


def merge_kernel(mine, theirs, own, sent):
    kept = mine.shape[1] // 2
    half = kept // 2
    rows = pl.ds(pl.multiple_of(half_kept() * kept, kept), kept)
    both = joined([mine[i, rows, :] for i in range(3)], [theirs[i, rows, :] for i in range(3)])
    odd = lax.axis_index("seq_1") % 2 == 1
    for i in range(3):
        at = pl.ds(i * half, half)
        own[at, :] = jnp.where(odd, both[i][half:], both[i][:half])
        sent[at, :] = jnp.where(odd, both[i][:half], both[i][half:])


def merge(mine, theirs):
    shape = jax.ShapeDtypeStruct((3 * mine.shape[1] // 4, mine.shape[2]), jnp.float32)
    return pl.pallas_call(
        merge_kernel,
        out_shape=(shape, shape),
        in_specs=[VMEM, VMEM],
        out_specs=(VMEM, VMEM),
        compiler_params=PARAMS,
        name="merge",
    )(mine, theirs)


def pack_kernel(mine, theirs, up_value, _, out):
    head_dim = mine.shape[1]
    half = mine.shape[0] // 3
    parts = [pl.ds(i * half, half) for i in range(3)]
    accum, _, total = joined([mine[p, :] for p in parts], [theirs[p, :] for p in parts])
    mean = accum / total
    value_map = up_value[lax.axis_index("grp")]
    value_map = jnp.where(
        half_kept() == 1, value_map[:, head_dim:], value_map[:, :head_dim]
    )
    wide = lax.dot_general(
        split(mean, 3), value_map, (((1,), (0,)), ((), ())), preferred_element_type=jnp.float32
    )
    extra = split(wide[2 * half :] + wide[half : 2 * half] + wide[:half], 2)
    rows = out.shape[1] - extra.shape[0]
    for b in range(out.shape[0]):
        out[b, rows:, :] = extra


def pack(mine, theirs, up_value, outgoing):
    return pl.pallas_call(
        pack_kernel,
        out_shape=jax.ShapeDtypeStruct(outgoing.shape, outgoing.dtype),
        in_specs=[VMEM] * 4,
        out_specs=VMEM,
        input_output_aliases={3: 0},
        compiler_params=PARAMS,
        name="pack",
    )(mine, theirs, up_value, pltpu.with_memory_space_constraint(outgoing, pltpu.VMEM))


def unpack_kernel(received, decode, attended, rows_out, sems, row_sems):
    cores, groups, high, wide, rows, rank = received.shape
    block_len = decode.shape[5]
    copies = []
    for c in range(cores):
        for y in range(high):
            for k in range(2):
                copies.append(
                    pltpu.make_async_copy(
                        received.at[c, :, y, :, pl.ds(k * block_len, block_len), :],
                        decode.at[0, :, :, y, c, :, pl.ds(k * rank, rank)],
                        sems.at[c, y, k],
                    )
                )
    for c in copies:
        c.start()
    half = (rows - 2 * block_len) // 2
    span = rows_out.shape[1] // groups
    for g in range(groups):
        for s in range(wide * high * cores):
            x, y, c = s // (high * cores), s // cores % high, s % cores
            seq = 2 * x + y // 2
            part = received[c, g, y, x, 2 * block_len :, :]
            part = part.astype(jnp.float32)
            part = part[half:] + part[:half]
            first = g * 16 + (c + y) % 2 * 8 + y % 2 * 4
            for j in range(half):
                at = (first + j) * rank
                rows_out[seq : seq + 1, at : at + rank] = part[j : j + 1]
        columns = pl.ds(g * span, span)
        copy = pltpu.make_async_copy(
            rows_out.at[:, columns], attended.at[:, columns], row_sems.at[g]
        )
        copy.start()
        copies.append(copy)
    for c in copies:
        c.wait()


def unpack(received, groups, batch, heads, block_len):
    _, rows, rank = received.shape
    received = received.reshape(2, groups, 4, 4, rows, rank)
    return pl.pallas_call(
        unpack_kernel,
        out_shape=(
            jax.ShapeDtypeStruct(
                (1, groups, 4, 4, 2, block_len, 2 * rank), received.dtype
            ),
            jax.ShapeDtypeStruct((batch, heads * rank), jnp.float32),
        ),
        in_specs=[VMEM],
        out_specs=(HBM, HBM),
        scratch_shapes=[
            pltpu.VMEM((batch, heads * rank), jnp.float32),
            pltpu.SemaphoreType.DMA((2, 4, 2)),
            pltpu.SemaphoreType.DMA((groups,)),
        ],
        compiler_params=PARAMS,
        name="unpack",
    )(received)


def swap(x, axes, mask):
    return lax.ppermute(x, axes, [(i, i ^ mask) for i in range(lax.axis_size(axes))])


def body(latent, up_key, up_value, queries, lengths, block_dest):
    groups = up_key.shape[0]
    block_len = latent.shape[2]
    batch, q_heads, _ = queries.shape
    part, lat = attend(latent[0], up_key, queries, lengths, 2)
    part, sent = merge(part, swap(part, "seq_2", 1))
    outgoing = slot(block_dest, lat, part, 8)
    outgoing = pack(part, swap(sent, ("seq_1", "seq_2"), 3), up_value, outgoing)
    received = lax.all_to_all(outgoing, EXCHANGE, split_axis=0, concat_axis=0, tiled=True)
    decode, attended = unpack(received, groups, batch, q_heads, block_len)
    return (decode.reshape(1, groups, -1, *latent.shape[2:]), attended)


def solution(mesh):
    finer = Mesh(
        mesh.devices.reshape(mesh.shape["grp"], 4, 4, 2), ("grp", "seq_0", "seq_1", "seq_2")
    )
    in_specs = (P("grp", SEQ, None, None), P(), P(), P(), P(), P())
    out_specs = (P(GRP_SEQ, None, None, None, None), P())
    return jax.shard_map(body, mesh=finer, in_specs=in_specs, out_specs=out_specs, check_vma=False)
```

```python
import jax
import jax.numpy as jnp
from jax import lax
from jax.experimental import pallas as pl
from jax.experimental.pallas import tpu as pltpu
from jax.sharding import Mesh
from jax.sharding import PartitionSpec as P

SEQ = ("seq_0", "seq_1", "seq_2")
GRP_SEQ = ("grp", "seq_0", "seq_1", "seq_2")
EXCHANGE = ("seq_2", "grp", "seq_1", "seq_0")
NEG = -1e30
VMEM = pl.BlockSpec(memory_space=pltpu.VMEM)
HBM = pl.BlockSpec(memory_space=pltpu.HBM)
PARAMS = pltpu.CompilerParams(vmem_limit_bytes=16 << 20)


def split(x, parts):
    pieces = []
    for _ in range(parts):
        piece = x.astype(jnp.bfloat16).astype(jnp.float32)
        pieces.append(piece)
        x = x - piece
    return jnp.concatenate(pieces, axis=0).astype(jnp.bfloat16)


def attend_kernel(ends, latent, up_key, queries, out, lat, key_map, query, lengths, sems):
    count, block_len, width = lat.shape
    chunks = sems.shape[0] - 3
    blocks = count // chunks
    tokens = blocks * block_len
    rank = width // 2
    heads, head_dim = query.shape
    per_group = key_map.shape[1] // head_dim
    per_kv = heads // per_group
    shard = lax.axis_index(SEQ)
    group = lax.axis_index("grp")
    quarter = lax.axis_size(SEQ) // queries.shape[0]
    seq = shard // quarter
    first = pl.multiple_of(group * heads, heads)
    small = [
        pltpu.make_async_copy(queries.at[seq, pl.ds(first, heads)], query, sems.at[0]),
        pltpu.make_async_copy(up_key.at[group], key_map, sems.at[1]),
        pltpu.make_async_copy(ends, lengths, sems.at[2]),
    ]
    parts = [pl.ds(i * blocks, blocks) for i in range(chunks)]
    large = [
        pltpu.make_async_copy(latent.at[part], lat.at[part], sems.at[3 + i])
        for i, part in enumerate(parts)
    ]
    for copy in small + large:
        copy.start()
    for copy in small:
        copy.wait()
    live_count = lengths[seq] - (shard % quarter) * (count * block_len)
    heads_f = query[...].astype(jnp.float32)
    rows = [
        lax.dot_general(
            heads_f[k * per_kv : (k + 1) * per_kv].astype(jnp.bfloat16),
            key_map[:, k * head_dim : (k + 1) * head_dim],
            (((1,), (1,)), ((), ())),
            preferred_element_type=jnp.float32,
        )
        for k in range(per_group)
    ]
    absorbed = split(jnp.concatenate(rows, axis=0) * (1.0 / float(head_dim) ** 0.5), 3)

    def scored(i):
        raw = lax.dot_general(
            absorbed,
            lat[parts[i], :, :rank].reshape(tokens, rank),
            (((1,), (1,)), ((), ())),
            preferred_element_type=jnp.float32,
        )
        scores = raw[2 * heads :] + raw[heads : 2 * heads] + raw[:heads]
        position = lax.broadcasted_iota(jnp.int32, (heads, tokens), 1) + i * tokens
        live = position < live_count
        return (jnp.where(live, scores, NEG), live)

    def weighed(scores, live):
        largest = jnp.max(scores, axis=1, keepdims=True)
        weights = jnp.where(live, jnp.exp(scores - largest), 0.0)
        return (split(weights, 2), largest, jnp.sum(weights, axis=1, keepdims=True))

    def summed(i, halves, largest, total):
        both = lax.dot_general(
            halves,
            lat[parts[i], :, rank:].reshape(tokens, rank),
            (((1,), (0,)), ((), ())),
            preferred_element_type=jnp.float32,
        )
        return (both[:heads] + both[heads:], largest, total)

    scores, weights, found = ({}, {}, [])
    for step in range(chunks + 2):
        if step < chunks:
            large[step].wait()
            scores[step] = scored(step)
        if 0 <= step - 1 < chunks:
            weights[step - 1] = weighed(*scores.pop(step - 1))
        if step >= 2:
            found.append(summed(step - 2, *weights.pop(step - 2)))
    largest = found[0][1]
    for chunk in found[1:]:
        largest = jnp.maximum(largest, chunk[1])
    factors = [jnp.exp(f[1] - largest) for f in found]
    out[0] = sum(f[0] * k for f, k in zip(found, factors))
    out[1] = jnp.broadcast_to(largest, (heads, rank))
    out[2] = jnp.broadcast_to(sum(f[2] * k for f, k in zip(found, factors)), (heads, rank))


def attend(latent, up_key, queries, lengths, chunks):
    heads = queries.shape[1] // up_key.shape[0]
    return pl.pallas_call(
        attend_kernel,
        out_shape=(
            jax.ShapeDtypeStruct((3, heads, latent.shape[2] // 2), jnp.float32),
            jax.ShapeDtypeStruct(latent.shape, latent.dtype),
        ),
        in_specs=[HBM] * 4,
        out_specs=(VMEM,) * 2,
        scratch_shapes=[
            pltpu.VMEM(up_key.shape[1:], up_key.dtype),
            pltpu.VMEM((heads, queries.shape[2]), queries.dtype),
            pltpu.SMEM(lengths.shape, jnp.int32),
            pltpu.SemaphoreType.DMA((3 + chunks,)),
        ],
        compiler_params=PARAMS,
        name="attend",
    )(*[in_hbm(x) for x in (lengths, latent, up_key, queries)])


def in_hbm(x):
    return pltpu.with_memory_space_constraint(x, pltpu.HBM)


def slot_kernel(dests, lat, up_value, after, outgoing, value_map, table, sems):
    count, block_len, width = lat.shape
    rank = width // 2
    first = pl.multiple_of(lax.axis_index(SEQ) * count, count)
    left = pl.multiple_of(half_kept() * value_map.shape[1], value_map.shape[1])
    copies = [
        pltpu.make_async_copy(dests.at[pl.ds(first, count)], table, sems.at[0]),
        pltpu.make_async_copy(
            up_value.at[lax.axis_index("grp"), :, pl.ds(left, value_map.shape[1])],
            value_map,
            sems.at[1],
        ),
    ]
    for copy in copies:
        copy.start()
    copies[0].wait()
    for b in range(count):
        d = table[b]
        to = (d & 1) * 64 + (d >> 5) * 16 + ((d >> 1) & 3) * 4 + ((d >> 3) & 3)
        outgoing[to, :block_len, :] = lat[b, :, :rank]
        outgoing[to, block_len : 2 * block_len, :] = lat[b, :, rank:]
    copies[1].wait()


def slot(block_dest, lat, up_value, after, extra):
    count, block_len, width = lat.shape
    return pl.pallas_call(
        slot_kernel,
        out_shape=(
            jax.ShapeDtypeStruct((count, 2 * block_len + extra, width // 2), lat.dtype),
            jax.ShapeDtypeStruct((up_value.shape[1], up_value.shape[2] // 2), up_value.dtype),
        ),
        in_specs=[HBM, VMEM, HBM, VMEM],
        out_specs=(VMEM, VMEM),
        scratch_shapes=[pltpu.SMEM((count,), jnp.int32), pltpu.SemaphoreType.DMA((2,))],
        compiler_params=PARAMS,
        name="slot",
    )(in_hbm(block_dest), lat, in_hbm(up_value), after)


def joined(first, second):
    largest = jnp.maximum(first[1], second[1])
    factor_a = jnp.exp(first[1] - largest)
    factor_b = jnp.exp(second[1] - largest)
    accum = first[0] * factor_a + second[0] * factor_b
    return (accum, largest, first[2] * factor_a + second[2] * factor_b)


def half_kept():
    return (lax.axis_index("seq_2") + lax.axis_index("seq_1")) % 2


def merge_kernel(mine, theirs, out):
    kept = out.shape[1]
    rows = pl.ds(pl.multiple_of(half_kept() * kept, kept), kept)
    both = joined(
        [mine[i, rows, :] for i in range(3)], [theirs[i, rows, :] for i in range(3)]
    )
    for i in range(3):
        out[i] = both[i]


def merge(mine, theirs):
    return pl.pallas_call(
        merge_kernel,
        out_shape=jax.ShapeDtypeStruct((3, mine.shape[1] // 2, mine.shape[2]), jnp.float32),
        in_specs=[VMEM, VMEM],
        out_specs=VMEM,
        compiler_params=PARAMS,
        name="merge",
    )(mine, theirs)


def pack_kernel(mine, theirs, value_map, _, out):
    accum, _, total = joined([mine[i] for i in range(3)], [theirs[i] for i in range(3)])
    mean = accum / total
    half = mean.shape[0] // 2
    mean = jnp.where(lax.axis_index("seq_1") % 2 == 1, mean[half:], mean[:half])
    wide = lax.dot_general(
        split(mean, 3), value_map[...], (((1,), (0,)), ((), ())), preferred_element_type=jnp.float32
    )
    extra = split(wide[2 * half :] + wide[half : 2 * half] + wide[:half], 2)
    rows = out.shape[1] - extra.shape[0]
    for b in range(out.shape[0]):
        out[b, rows:, :] = extra


def pack(mine, theirs, value_map, outgoing):
    return pl.pallas_call(
        pack_kernel,
        out_shape=jax.ShapeDtypeStruct(outgoing.shape, outgoing.dtype),
        in_specs=[VMEM] * 4,
        out_specs=VMEM,
        input_output_aliases={3: 0},
        compiler_params=PARAMS,
        name="pack",
    )(mine, theirs, value_map, pltpu.with_memory_space_constraint(outgoing, pltpu.VMEM))


def unpack_kernel(received, decode, attended, rows_out, sems, row_sems):
    cores, groups, high, wide, rows, rank = received.shape
    block_len = decode.shape[5]
    copies = []
    for c in range(cores):
        for y in range(high):
            for k in range(2):
                copies.append(
                    pltpu.make_async_copy(
                        received.at[c, :, y, :, pl.ds(k * block_len, block_len), :],
                        decode.at[0, :, :, y, c, :, pl.ds(k * rank, rank)],
                        sems.at[c, y, k],
                    )
                )
    for c in copies:
        c.start()
    half = (rows - 2 * block_len) // 2
    span = rows_out.shape[1] // groups
    for g in range(groups):
        for s in range(wide * high * cores):
            x, y, c = s // (high * cores), s // cores % high, s % cores
            seq = 2 * x + y // 2
            part = received[c, g, y, x, 2 * block_len :, :]
            part = part.astype(jnp.float32)
            part = part[half:] + part[:half]
            first = g * 16 + (c + y) % 2 * 8 + y % 2 * 4
            for j in range(half):
                at = (first + j) * rank
                rows_out[seq : seq + 1, at : at + rank] = part[j : j + 1]
        columns = pl.ds(g * span, span)
        copy = pltpu.make_async_copy(
            rows_out.at[:, columns], attended.at[:, columns], row_sems.at[g]
        )
        copy.start()
        copies.append(copy)
    for c in copies:
        c.wait()


def unpack(received, groups, batch, heads, block_len):
    _, rows, rank = received.shape
    received = received.reshape(2, groups, 4, 4, rows, rank)
    return pl.pallas_call(
        unpack_kernel,
        out_shape=(
            jax.ShapeDtypeStruct(
                (1, groups, 4, 4, 2, block_len, 2 * rank), received.dtype
            ),
            jax.ShapeDtypeStruct((batch, heads * rank), jnp.float32),
        ),
        in_specs=[VMEM],
        out_specs=(HBM, HBM),
        scratch_shapes=[
            pltpu.VMEM((batch, heads * rank), jnp.float32),
            pltpu.SemaphoreType.DMA((2, 4, 2)),
            pltpu.SemaphoreType.DMA((groups,)),
        ],
        compiler_params=PARAMS,
        name="unpack",
    )(received)


def swap(x, axes, mask):
    return lax.ppermute(x, axes, [(i, i ^ mask) for i in range(lax.axis_size(axes))])


def body(latent, up_key, up_value, queries, lengths, block_dest):
    groups = up_key.shape[0]
    block_len = latent.shape[2]
    batch, q_heads, _ = queries.shape
    part, lat = attend(latent[0], up_key, queries, lengths, 2)
    part = merge(part, swap(part, "seq_2", 1))
    outgoing, value_map = slot(block_dest, lat, up_value, part, 8)
    outgoing = pack(part, swap(part, ("seq_1", "seq_2"), 3), value_map, outgoing)
    received = lax.all_to_all(outgoing, EXCHANGE, split_axis=0, concat_axis=0, tiled=True)
    decode, attended = unpack(received, groups, batch, q_heads, block_len)
    return (decode.reshape(1, groups, -1, *latent.shape[2:]), attended)


def solution(mesh):
    finer = Mesh(
        mesh.devices.reshape(mesh.shape["grp"], 4, 4, 2), ("grp", "seq_0", "seq_1", "seq_2")
    )
    in_specs = (P("grp", SEQ, None, None), P(), P(), P(), P(), P())
    out_specs = (P(GRP_SEQ, None, None, None, None), P())
    return jax.shard_map(body, mesh=finer, in_specs=in_specs, out_specs=out_specs, check_vma=False)
```

```python
import jax
import jax.numpy as jnp
from jax import lax
from jax.experimental import pallas as pl
from jax.experimental.pallas import tpu as pltpu
from jax.sharding import Mesh
from jax.sharding import PartitionSpec as P

SEQ = ("seq_0", "seq_1", "seq_2")
GRP_SEQ = ("grp", "seq_0", "seq_1", "seq_2")
EXCHANGE = ("seq_2", "grp", "seq_1", "seq_0")
NEG = -1e30
VMEM = pl.BlockSpec(memory_space=pltpu.VMEM)
HBM = pl.BlockSpec(memory_space=pltpu.HBM)
PARAMS = pltpu.CompilerParams(vmem_limit_bytes=16 << 20)


def split(x, parts):
    pieces = []
    for _ in range(parts):
        piece = x.astype(jnp.bfloat16).astype(jnp.float32)
        pieces.append(piece)
        x = x - piece
    return jnp.concatenate(pieces, axis=0).astype(jnp.bfloat16)


def attend_kernel(ends, latent, up_key, queries, out, lat, key_map, query, lengths, sems):
    count, block_len, width = lat.shape
    chunks = sems.shape[0] - 3
    blocks = count // chunks
    tokens = blocks * block_len
    rank = width // 2
    heads, head_dim = query.shape
    per_group = key_map.shape[1] // head_dim
    per_kv = heads // per_group
    shard = lax.axis_index(SEQ)
    group = lax.axis_index("grp")
    quarter = lax.axis_size(SEQ) // queries.shape[0]
    seq = shard // quarter
    first = pl.multiple_of(group * heads, heads)
    small = [
        pltpu.make_async_copy(queries.at[seq, pl.ds(first, heads)], query, sems.at[0]),
        pltpu.make_async_copy(up_key.at[group], key_map, sems.at[1]),
        pltpu.make_async_copy(ends, lengths, sems.at[2]),
    ]
    parts = [pl.ds(i * blocks, blocks) for i in range(chunks)]
    large = [
        pltpu.make_async_copy(latent.at[part], lat.at[part], sems.at[3 + i])
        for i, part in enumerate(parts)
    ]
    for copy in small + large:
        copy.start()
    for copy in small:
        copy.wait()
    live_count = lengths[seq] - (shard % quarter) * (count * block_len)
    heads_f = query[...].astype(jnp.float32)
    rows = [
        lax.dot_general(
            heads_f[k * per_kv : (k + 1) * per_kv].astype(jnp.bfloat16),
            key_map[:, k * head_dim : (k + 1) * head_dim],
            (((1,), (1,)), ((), ())),
            preferred_element_type=jnp.float32,
        )
        for k in range(per_group)
    ]
    absorbed = split(jnp.concatenate(rows, axis=0) * (1.0 / float(head_dim) ** 0.5), 3)

    def scored(i):
        raw = lax.dot_general(
            absorbed,
            lat[parts[i], :, :rank].reshape(tokens, rank),
            (((1,), (1,)), ((), ())),
            preferred_element_type=jnp.float32,
        )
        scores = raw[2 * heads :] + raw[heads : 2 * heads] + raw[:heads]
        position = lax.broadcasted_iota(jnp.int32, (heads, tokens), 1) + i * tokens
        live = position < live_count
        return (jnp.where(live, scores, NEG), live)

    def weighed(scores, live):
        largest = jnp.max(scores, axis=1, keepdims=True)
        weights = jnp.where(live, jnp.exp(scores - largest), 0.0)
        return (split(weights, 2), largest, jnp.sum(weights, axis=1, keepdims=True))

    def summed(i, halves, largest, total):
        both = lax.dot_general(
            halves,
            lat[parts[i], :, rank:].reshape(tokens, rank),
            (((1,), (0,)), ((), ())),
            preferred_element_type=jnp.float32,
        )
        return (both[:heads] + both[heads:], largest, total)

    scores, weights, found = ({}, {}, [])
    for step in range(chunks + 2):
        if step < chunks:
            large[step].wait()
            scores[step] = scored(step)
        if 0 <= step - 1 < chunks:
            weights[step - 1] = weighed(*scores.pop(step - 1))
        if step >= 2:
            found.append(summed(step - 2, *weights.pop(step - 2)))
    largest = found[0][1]
    for chunk in found[1:]:
        largest = jnp.maximum(largest, chunk[1])
    factors = [jnp.exp(f[1] - largest) for f in found]
    out[0] = sum(f[0] * k for f, k in zip(found, factors))
    out[1] = jnp.broadcast_to(largest, (heads, rank))
    out[2] = jnp.broadcast_to(sum(f[2] * k for f, k in zip(found, factors)), (heads, rank))


def attend(latent, up_key, queries, lengths, chunks):
    heads = queries.shape[1] // up_key.shape[0]
    return pl.pallas_call(
        attend_kernel,
        out_shape=(
            jax.ShapeDtypeStruct((3, heads, latent.shape[2] // 2), jnp.float32),
            jax.ShapeDtypeStruct(latent.shape, latent.dtype),
        ),
        in_specs=[HBM] * 4,
        out_specs=(VMEM,) * 2,
        scratch_shapes=[
            pltpu.VMEM(up_key.shape[1:], up_key.dtype),
            pltpu.VMEM((heads, queries.shape[2]), queries.dtype),
            pltpu.SMEM(lengths.shape, jnp.int32),
            pltpu.SemaphoreType.DMA((3 + chunks,)),
        ],
        compiler_params=PARAMS,
        name="attend",
    )(*[in_hbm(x) for x in (lengths, latent, up_key, queries)])


def in_hbm(x):
    return pltpu.with_memory_space_constraint(x, pltpu.HBM)


def slot_kernel(dests, lat, up_value, after, outgoing, value_map, table, sems):
    count, block_len, width = lat.shape
    rank = width // 2
    first = pl.multiple_of(lax.axis_index(SEQ) * count, count)
    left = pl.multiple_of(half_kept() * value_map.shape[1], value_map.shape[1])
    copies = [
        pltpu.make_async_copy(dests.at[pl.ds(first, count)], table, sems.at[0]),
        pltpu.make_async_copy(
            up_value.at[lax.axis_index("grp"), :, pl.ds(left, value_map.shape[1])],
            value_map,
            sems.at[1],
        ),
    ]
    for copy in copies:
        copy.start()
    copies[0].wait()
    for b in range(count):
        d = table[b]
        to = (d & 1) * 64 + (d >> 5) * 16 + ((d >> 1) & 3) * 4 + ((d >> 3) & 3)
        outgoing[to, :block_len, :] = lat[b, :, :rank]
        outgoing[to, block_len : 2 * block_len, :] = lat[b, :, rank:]
    copies[1].wait()


def slot(block_dest, lat, up_value, after, extra):
    count, block_len, width = lat.shape
    return pl.pallas_call(
        slot_kernel,
        out_shape=(
            jax.ShapeDtypeStruct((count, 2 * block_len + extra, width // 2), lat.dtype),
            jax.ShapeDtypeStruct((up_value.shape[1], up_value.shape[2] // 2), up_value.dtype),
        ),
        in_specs=[HBM, VMEM, HBM, VMEM],
        out_specs=(VMEM, VMEM),
        scratch_shapes=[pltpu.SMEM((count,), jnp.int32), pltpu.SemaphoreType.DMA((2,))],
        compiler_params=PARAMS,
        name="slot",
    )(in_hbm(block_dest), lat, in_hbm(up_value), after)


def joined(first, second):
    largest = jnp.maximum(first[1], second[1])
    factor_a = jnp.exp(first[1] - largest)
    factor_b = jnp.exp(second[1] - largest)
    accum = first[0] * factor_a + second[0] * factor_b
    return (accum, largest, first[2] * factor_a + second[2] * factor_b)


def half_kept():
    return (lax.axis_index("seq_2") + lax.axis_index("seq_1")) % 2


def merge_kernel(mine, theirs, own, sent):
    kept = mine.shape[1] // 2
    half = kept // 2
    rows = pl.ds(pl.multiple_of(half_kept() * kept, kept), kept)
    both = joined([mine[i, rows, :] for i in range(3)], [theirs[i, rows, :] for i in range(3)])
    odd = lax.axis_index("seq_1") % 2 == 1
    for i in range(3):
        at = pl.ds(i * half, half)
        own[at, :] = jnp.where(odd, both[i][half:], both[i][:half])
        sent[at, :] = jnp.where(odd, both[i][:half], both[i][half:])


def merge(mine, theirs):
    shape = jax.ShapeDtypeStruct((3 * mine.shape[1] // 4, mine.shape[2]), jnp.float32)
    return pl.pallas_call(
        merge_kernel,
        out_shape=(shape, shape),
        in_specs=[VMEM, VMEM],
        out_specs=(VMEM, VMEM),
        compiler_params=PARAMS,
        name="merge",
    )(mine, theirs)


def pack_kernel(mine, theirs, value_map, _, out):
    half = mine.shape[0] // 3
    parts = [pl.ds(i * half, half) for i in range(3)]
    accum, _, total = joined([mine[p, :] for p in parts], [theirs[p, :] for p in parts])
    mean = accum / total
    wide = lax.dot_general(
        split(mean, 3), value_map[...], (((1,), (0,)), ((), ())), preferred_element_type=jnp.float32
    )
    extra = split(wide[2 * half :] + wide[half : 2 * half] + wide[:half], 2)
    rows = out.shape[1] - extra.shape[0]
    for b in range(out.shape[0]):
        out[b, rows:, :] = extra


def pack(mine, theirs, value_map, outgoing):
    return pl.pallas_call(
        pack_kernel,
        out_shape=jax.ShapeDtypeStruct(outgoing.shape, outgoing.dtype),
        in_specs=[VMEM] * 4,
        out_specs=VMEM,
        input_output_aliases={3: 0},
        compiler_params=PARAMS,
        name="pack",
    )(mine, theirs, value_map, pltpu.with_memory_space_constraint(outgoing, pltpu.VMEM))


def unpack_kernel(received, decode, attended, rows_out, sems, row_sems):
    cores, groups, high, wide, rows, rank = received.shape
    block_len = decode.shape[5]
    copies = []
    for c in range(cores):
        for y in range(high):
            for k in range(2):
                copies.append(
                    pltpu.make_async_copy(
                        received.at[c, :, y, :, pl.ds(k * block_len, block_len), :],
                        decode.at[0, :, :, y, c, :, pl.ds(k * rank, rank)],
                        sems.at[c, y, k],
                    )
                )
    for c in copies:
        c.start()
    half = (rows - 2 * block_len) // 2
    span = rows_out.shape[1] // groups
    for g in range(groups):
        for s in range(wide * high * cores):
            x, y, c = s // (high * cores), s // cores % high, s % cores
            seq = 2 * x + y // 2
            part = received[c, g, y, x, 2 * block_len :, :]
            part = part.astype(jnp.float32)
            part = part[half:] + part[:half]
            first = g * 16 + (c + y) % 2 * 8 + y % 2 * 4
            for j in range(half):
                at = (first + j) * rank
                rows_out[seq : seq + 1, at : at + rank] = part[j : j + 1]
        columns = pl.ds(g * span, span)
        copy = pltpu.make_async_copy(
            rows_out.at[:, columns], attended.at[:, columns], row_sems.at[g]
        )
        copy.start()
        copies.append(copy)
    for c in copies:
        c.wait()


def unpack(received, groups, batch, heads, block_len):
    _, rows, rank = received.shape
    received = received.reshape(2, groups, 4, 4, rows, rank)
    return pl.pallas_call(
        unpack_kernel,
        out_shape=(
            jax.ShapeDtypeStruct(
                (1, groups, 4, 4, 2, block_len, 2 * rank), received.dtype
            ),
            jax.ShapeDtypeStruct((batch, heads * rank), jnp.float32),
        ),
        in_specs=[VMEM],
        out_specs=(HBM, HBM),
        scratch_shapes=[
            pltpu.VMEM((batch, heads * rank), jnp.float32),
            pltpu.SemaphoreType.DMA((2, 4, 2)),
            pltpu.SemaphoreType.DMA((groups,)),
        ],
        compiler_params=PARAMS,
        name="unpack",
    )(received)


def swap(x, axes, mask):
    return lax.ppermute(x, axes, [(i, i ^ mask) for i in range(lax.axis_size(axes))])


def body(latent, up_key, up_value, queries, lengths, block_dest):
    groups = up_key.shape[0]
    block_len = latent.shape[2]
    batch, q_heads, _ = queries.shape
    part, lat = attend(latent[0], up_key, queries, lengths, 2)
    part, sent = merge(part, swap(part, "seq_2", 1))
    outgoing, value_map = slot(block_dest, lat, up_value, part, 8)
    outgoing = pack(part, swap(sent, ("seq_1", "seq_2"), 3), value_map, outgoing)
    received = lax.all_to_all(outgoing, EXCHANGE, split_axis=0, concat_axis=0, tiled=True)
    decode, attended = unpack(received, groups, batch, q_heads, block_len)
    return (decode.reshape(1, groups, -1, *latent.shape[2:]), attended)


def solution(mesh):
    finer = Mesh(
        mesh.devices.reshape(mesh.shape["grp"], 4, 4, 2), ("grp", "seq_0", "seq_1", "seq_2")
    )
    in_specs = (P("grp", SEQ, None, None), P(), P(), P(), P(), P())
    out_specs = (P(GRP_SEQ, None, None, None, None), P())
    return jax.shard_map(body, mesh=finer, in_specs=in_specs, out_specs=out_specs, check_vma=False)
```
